32 devices in a mesh: grow: 16 (over z, y, x), lat: 2 (over core).
Axes of the slice: x: 2, y: 2, z: 4, core: 2. Of those that a mesh axis runs over, the one named last changes fastest.
Arguments:
- labels: int32 [128, 64, 256], P('grow', 'lat'), may hold values from 0 to 3
- seed_blend: float32 [4, 128, 64, 256], P(None, 'grow', 'lat'), may hold values from 0.02 to 0.6
- potential: float32 [2, 128, 64, 256], P(None, 'grow', 'lat'), may hold values from -3 to 3
- inflow_index: int32 [8, 64, 256], P(None, 'lat'), may hold values from 0 to 15
- liquid_table: float32 [16, 2], replicated, may hold values from -1 to 1
Outputs:
- phase_field: float32 [4, 128, 64, 256], P(None, 'grow', 'lat')
- chem_field: float32 [2, 128, 64, 256], P(None, 'grow', 'lat')
The draws below stay inside these ranges and needn't reach their ends.
All inputs are finite; a program needn't handle non-finite values.
Results may differ from the reference program's by a relative error of at most 0.0001.
Values sent between devices are 32-bit elements; how exact they have to be, the bound alone decides.
A program may use at most 64 MiB of HBM per device.

```python
import math
import jax
import jax.numpy as jnp

CZ = 8
NY = 256
LIQUIDS = 16
GROWTH_PLANES = 128
NX = 64


def with_ends(values, rng, smallest, high):
    spot = [jax.random.randint(jax.random.fold_in(rng, axis), (), 0, length) for axis, length in enumerate(values.shape)]
    widest = values.shape.index(max(values.shape))
    neighbour = spot[:widest] + [(spot[widest] + 1) % values.shape[widest]] + spot[widest + 1:]
    return values.at[tuple(spot)].set(smallest).at[tuple(neighbour)].set(high)


def steps_of(stream_key, extent, split, smallest, top_value):
    gain, own = 1.0, jax.random.fold_in(stream_key, 6)
    for dim, shards_of in split:
        draws = jnp.exp(jax.random.uniform(jax.random.fold_in(own, dim), (shards_of,), jnp.float32, smallest / len(split), top_value / len(split)))
        gain = gain * jnp.repeat(draws, extent[dim] // shards_of).reshape([-1 if axis == dim else 1 for axis in range(len(extent))])
    return gain


def gaussian(stream_key, dims, width, bound, pieces=(), kind=jnp.bfloat16):
    values = width * jax.random.normal(stream_key, dims, jnp.float32)
    if pieces:
        values = values * steps_of(stream_key, dims, pieces, -0.22, 0.18)
    return jnp.clip(values, -bound, bound).astype(kind)


def setup_inputs(seed: int = 0) -> dict:
    arg_keys = jax.random.split(jax.random.key(seed), 6)
    return {
        "labels": with_ends(jax.random.randint(arg_keys[0], (GROWTH_PLANES, NX, NY), 0, 4), jax.random.fold_in(arg_keys[0], 1), 0, 3).astype(jnp.int32),
        "seed_blend": jnp.clip(jnp.exp(math.log(0.6) - 3.4011974 * jax.random.uniform(arg_keys[1], (4, GROWTH_PLANES, NX, NY), jnp.float32) ** steps_of(arg_keys[1], (4, GROWTH_PLANES, NX, NY), ((1, 16), (2, 2)), -0.2, 0.2)), 0.02, 0.6),
        "potential": gaussian(arg_keys[2], (2, GROWTH_PLANES, NX, NY), 0.5, 3.0, ((1, 16), (2, 2)), jnp.float32),
        "inflow_index": with_ends(jax.random.randint(arg_keys[3], (CZ, NX, NY), 0, LIQUIDS), jax.random.fold_in(arg_keys[3], 1), 0, LIQUIDS - 1).astype(jnp.int32),
        "liquid_table": jnp.clip(jax.random.uniform(arg_keys[4], (LIQUIDS, 2), jnp.float32, -1.0, 1.0), -1.0, 1.0),
    }


offset_table = ((0.0, 0.0), (0.6, -0.3), (-0.4, 0.5), (-0.2, -0.6))
latent_heat = (0.0, 0.8, 0.8, 0.8)
relax_rate = 0.1
diffusion = 0.05


def evolve_fields(padded_fields, thermal_profile):
    centre = padded_fields[:, 1:-1, 1:-1]
    laplace = (padded_fields[:, 2:, 1:-1] + padded_fields[:, :-2, 1:-1]) + (padded_fields[:, 1:-1, 2:] + padded_fields[:, 1:-1, :-2])
    laplace = laplace + (jnp.roll(centre, -1, axis=3) + jnp.roll(centre, 1, axis=3)) - 6.0 * centre
    phases = centre[:4]
    chemical = centre[4:]
    offsets = jnp.array(offset_table, jnp.float32)
    latent_release = jnp.array(latent_heat, jnp.float32)[:, None, None, None]
    free_energy_density = jnp.zeros_like(phases)
    for solute in range(2):
        shifted = chemical[solute][None] + offsets[:, solute][:, None, None, None]
        free_energy_density = free_energy_density + shifted * shifted
    free_energy_density = -0.5 * free_energy_density + latent_release * thermal_profile
    driving = laplace[:4] - phases * (1.0 - phases) * (1.0 - 2.0 * phases) - 2.0 * phases * free_energy_density
    driving = driving - jnp.mean(driving, axis=0, keepdims=True)
    new_phases = phases + relax_rate * driving
    growth = new_phases * new_phases - phases * phases
    susceptible = jnp.sum(new_phases * new_phases, axis=0)
    mobile = diffusion * (0.1 + new_phases[0] * new_phases[0])
    new_chemical = []
    for solute in range(2):
        shifted = chemical[solute][None] + offsets[:, solute][:, None, None, None]
        source = jnp.sum(shifted * growth, axis=0)
        new_chemical.append(chemical[solute] + (mobile * laplace[4 + solute] - source) / susceptible)
    return jnp.concatenate([new_phases, jnp.stack(new_chemical)], axis=0)


def initial(labels, seed_blend, potential):
    kinds = jnp.arange(4, dtype=jnp.int32)[:, None, None, None]
    onehot = (labels[None] == kinds).astype(jnp.float32)
    phases = (onehot + seed_blend) / (1.0 + jnp.sum(seed_blend, axis=0))
    return jnp.concatenate([phases, potential], axis=0)


def inflow_fields(inflow_index, liquid_table):
    kinds = jnp.arange(liquid_table.shape[0], dtype=jnp.int32)[:, None, None, None]
    selected = (inflow_index[None] == kinds).astype(jnp.float32)
    chemical = []
    for solute in range(2):
        chemical.append(jnp.sum(selected * liquid_table[:, solute][:, None, None, None], axis=0))
    liquid = jnp.ones_like(chemical[0])
    solid = jnp.zeros_like(chemical[0])
    return jnp.stack([liquid, solid, solid, solid, chemical[0], chemical[1]])


def reference(labels, seed_blend, potential, inflow_index, liquid_table):
    field_arrays = initial(labels, seed_blend, potential)
    grid_planes = jnp.arange(GROWTH_PLANES, dtype=jnp.int32).astype(jnp.float32)
    thermal_profile = ((2.0 * (grid_planes + 0.5)) / float(GROWTH_PLANES) - 1.0)[:, None, None]
    for turn in range(2):
        padded_fields = jnp.concatenate([field_arrays[:, :1], field_arrays, field_arrays[:, -1:]], axis=1)
        padded_fields = jnp.concatenate([padded_fields[:, :, -1:], padded_fields, padded_fields[:, :, :1]], axis=2)
        field_arrays = evolve_fields(padded_fields, thermal_profile)
    result = jnp.concatenate([field_arrays[:, CZ:], inflow_fields(inflow_index, liquid_table)], axis=1)
    return result[:4], result[4:]
```

```python
import functools

import jax
import jax.numpy as jnp
from jax import lax
from jax.experimental import pallas as pl
from jax.experimental.pallas import tpu as pltpu
from jax.sharding import PartitionSpec as P

offset_table = ((0.0, 0.0), (0.6, -0.3), (-0.4, 0.5), (-0.2, -0.6))
latent_heat = (0.0, 0.8, 0.8, 0.8)
relax_rate = 0.1
diffusion = 0.05
MESH = pl.DeviceIdType.MESH
ROWS = 8


def advance(phi, chem, lap, temp):
    phi = list(phi) + [1.0 - (phi[0] + phi[1] + phi[2])]
    square = chem[0] * chem[0] + chem[1] * chem[1]
    pull = []
    for a in range(4):
        e0, e1 = offset_table[a]
        p = phi[a]
        w = square - (1.0 - p) * (1.0 - 2.0 * p)
        if a:
            w = w + ((2.0 * e0) * chem[0] + (2.0 * e1) * chem[1] + ((e0 * e0 + e1 * e1) - 2.0 * latent_heat[a] * temp))
        pull.append(p * w)
    mean = 0.25 * ((pull[0] + pull[1]) + (pull[2] + pull[3]))
    new = [phi[a] + relax_rate * ((lap[a] + pull[a]) - mean) for a in range(3)]
    new.append(1.0 - (new[0] + new[1] + new[2]))
    squares = [v * v for v in new]
    growth = [squares[a] - phi[a] * phi[a] for a in range(4)]
    total = (growth[0] + growth[1]) + (growth[2] + growth[3])
    inverse = 1.0 / ((squares[0] + squares[1]) + (squares[2] + squares[3]))
    mobile = diffusion * (0.1 + squares[0])
    out = []
    for k in range(2):
        source = chem[k] * total
        for a in range(1, 4):
            source = source + offset_table[a][k] * growth[a]
        out.append(chem[k] + (mobile * lap[3 + k] - source) * inverse)
    return new, out


def kernel(n, m, labels_h, blend_h, chem_h, index_h, table_h, phase_out, chem_out,
           table, labels, blend, index, own, g, half, from_right, from_left, staged,
           load_sem, send_sem, plane_send, recv_sem, plane_recv, lat_send, lat_recv, out_sem):
    cz, nx, ny = labels.shape
    tiles = nx // ROWS
    me = lax.axis_index("grow")
    lat = lax.axis_index("lat")
    right, left = lax.rem(lat + 1, m), lax.rem(lat + m - 1, m)
    even = lax.rem(me, 2) == 0
    gives, gives_end = me > 0, me > 1
    gets, gets_end = me < n - 1, me < n - 2
    row = lax.broadcasted_iota(jnp.int32, (ROWS, ny), 0)

    loads = [
        pltpu.make_async_copy(labels_h, labels, load_sem.at[0]),
        pltpu.make_async_copy(blend_h, blend, load_sem.at[1]),
        pltpu.make_async_copy(index_h, index, load_sem.at[2]),
        pltpu.make_async_copy(chem_h.at[:, cz - 2 : cz], g.at[3:5, 0:2, 0:nx], load_sem.at[3]),
        pltpu.make_async_copy(table_h, table, load_sem.at[4]),
    ]
    for load in loads:
        load.start()

    barrier = pltpu.get_barrier_semaphore()
    met = jnp.int32(2)
    for step in (-2, -1, 1, 2):
        there = jnp.logical_and(me + step >= 0, me + step < n)
        met = met + there.astype(jnp.int32)

        @pl.when(there)
        def _():
            pl.semaphore_signal(barrier, inc=1, device_id={"grow": me + step}, device_id_type=MESH)

    for side in (left, right):
        pl.semaphore_signal(barrier, inc=1, device_id={"lat": side}, device_id_type=MESH)
    pl.semaphore_wait(barrier, met)

    below, below2 = lax.rem(me + n - 1, n), lax.rem(me + 2 * n - 2, n)
    above = lax.rem(me + 1, n)

    def along(src, dst, send, recv, device):
        return pltpu.make_async_remote_copy(
            src_ref=src, dst_ref=dst, send_sem=send, recv_sem=recv,
            device_id={"grow": device}, device_id_type=MESH)

    end_chem = along(chem_h.at[:, 0:2], g.at[3:5, cz + 2 : cz + 4, 0:nx], send_sem.at[0], recv_sem.at[0], below2)
    end_phi = along(own.at[:, 0:2], g.at[0:3, cz + 2 : cz + 4, 0:nx], send_sem.at[1], recv_sem.at[1], below2)
    head_chem = along(chem_h.at[:, 0:2], g.at[3:5, 2:4, 0:nx], send_sem.at[2], recv_sem.at[2], below)
    head_phi = along(own.at[:, 0:2], g.at[0:3, 2:4, 0:nx], send_sem.at[3], recv_sem.at[3], below)
    body_chem = along(chem_h.at[:, 2:cz], g.at[3:5, 4 : cz + 2, 0:nx], send_sem.at[4], recv_sem.at[4], below)
    pass_chem = along(g.at[3:5, cz + 2 : cz + 4, 0:nx], g.at[3:5, 2:4, 0:nx], send_sem.at[5], recv_sem.at[2], above)
    pass_phi = along(g.at[0:3, cz + 2 : cz + 4, 0:nx], g.at[0:3, 2:4, 0:nx], send_sem.at[6], recv_sem.at[3], above)

    def plane_phi(p):
        return along(own.at[:, pl.ds(p, 1)], g.at[0:3, pl.ds(p + 2, 1), 0:nx], plane_send.at[p], plane_recv.at[p], below)

    odd_gives = jnp.logical_and(gives, jnp.logical_not(even))

    @pl.when(gives_end)
    def _():
        end_chem.start()

    @pl.when(odd_gives)
    def _():
        head_chem.start()

    @pl.when(gives)
    def _():
        body_chem.start()

    loads[0].wait()
    loads[1].wait()

    def initial(p, _):
        kind = labels[p]
        weights = [blend[a, p] for a in range(4)]
        inverse = 1.0 / (1.0 + ((weights[0] + weights[1]) + (weights[2] + weights[3])))
        for a in range(3):
            own[a, p] = (jnp.where(kind == a, 1.0, 0.0) + weights[a]) * inverse
        return _

    lax.fori_loop(0, cz, initial, None)
    for k in range(2):
        for a in range(3):
            g[a, k, 0:nx] = own[a, cz - 2 + k]

    @pl.when(gives_end)
    def _():
        end_phi.start()

    @pl.when(odd_gives)
    def _():
        head_phi.start()

    @pl.when(gives)
    def _():
        def go(p, _):
            plane_phi(p).start()
            return _

        lax.fori_loop(2, cz, go, None)

    loads[2].wait()
    loads[3].wait()
    loads[4].wait()

    def sideways(fields, planes, group):
        return (
            pltpu.make_async_remote_copy(
                src_ref=g.at[fields, planes, nx - ROWS : nx], dst_ref=from_left.at[fields, planes],
                send_sem=lat_send.at[0, group], recv_sem=lat_recv.at[0, group],
                device_id={"lat": right}, device_id_type=MESH),
            pltpu.make_async_remote_copy(
                src_ref=g.at[fields, planes, 0:ROWS], dst_ref=from_right.at[fields, planes],
                send_sem=lat_send.at[1, group], recv_sem=lat_recv.at[1, group],
                device_id={"lat": left}, device_id_type=MESH),
        )

    everything, phases, chemical = slice(0, 5), slice(0, 3), slice(3, 5)
    lat_own = sideways(everything, slice(0, 2), 0)
    lat_head = sideways(everything, slice(2, 4), 1)
    lat_end = sideways(everything, slice(cz + 2, cz + 4), 2)
    lat_chem = sideways(chemical, slice(4, cz + 2), 3)

    def lat_plane(p):
        return sideways(phases, pl.ds(p + 2, 1), 4 + p)

    def start(pair):
        for copy in pair:
            copy.start()

    def wait(pair):
        for copy in pair:
            copy.wait()

    def merge(fields, z):
        for f in fields:
            g[f, z, nx : nx + ROWS] = jnp.where(row < 4, from_right[f, z], from_left[f, z])

    def tile_step(src, z, t):
        def part(f, z, t):
            return src[f, z, t * ROWS : (t + 1) * ROWS]

        after, before = (t + 1) % (tiles + 1), (t + tiles) % (tiles + 1)
        centre, lap = [], []
        for f in range(5):
            c = part(f, z, t)
            up = pltpu.roll(jnp.where(row == 0, part(f, z, after), c), ROWS - 1, 0)
            down = pltpu.roll(jnp.where(row == ROWS - 1, part(f, z, before), c), 1, 0)
            lap.append(
                ((part(f, z + 1, t) + part(f, z - 1, t)) + (up + down))
                + (pltpu.roll(c, ny - 1, 1) + pltpu.roll(c, 1, 1)) - 6.0 * c)
            centre.append(c)
        plane = ((me + 1) * cz - 2 + z).astype(jnp.float32)
        temp = 2.0 * (plane + 0.5) / float(n * cz) - 1.0
        return advance(centre[:3], centre[3:], lap, temp)

    def first(z):
        for t in range(tiles + 1):
            new, chem = tile_step(g, z, t)
            for f, value in enumerate(new[:3] + chem):
                half[f, z, t * ROWS : (t + 1) * ROWS] = value

    def put(o):
        return (
            pltpu.make_async_copy(staged.at[0:4, pl.ds(o, 1)], phase_out.at[:, pl.ds(o, 1)], out_sem.at[0, o]),
            pltpu.make_async_copy(staged.at[4:6, pl.ds(o, 1)], chem_out.at[:, pl.ds(o, 1)], out_sem.at[1, o]),
        )

    def second(z):
        for t in range(tiles):
            new, chem = tile_step(half, z, t)
            for f, value in enumerate(new + chem):
                staged[f, z - 2, t * ROWS : (t + 1) * ROWS] = value
        start(put(z - 2))

    def firsts(low, high):
        lax.fori_loop(low, high, lambda z, _: first(z), None)

    def seconds(low, high):
        lax.fori_loop(low, high, lambda z, _: second(z), None)

    @pl.when(gets)
    def _():
        start(lat_own)

        @pl.when(jnp.logical_and(even, gets_end))
        def _():
            end_chem.wait_recv()
            pass_chem.start()
            end_phi.wait_recv()
            pass_phi.start()
            start(lat_end)

        @pl.when(even)
        def _():
            head_chem.wait_recv()
            head_phi.wait_recv()
            start(lat_head)

        body_chem.wait_recv()
        start(lat_chem)
        wait(lat_own)
        for z in (0, 1):
            merge(range(5), z)

        @pl.when(even)
        def _():
            wait(lat_head)
            for z in (2, 3):
                merge(range(5), z)
            firsts(1, 3)

        wait(lat_chem)
        lax.fori_loop(4, cz + 2, lambda z, _: merge((3, 4), z), None)

        def plane(p, _):
            z = p + 2
            plane_phi(p).wait_recv()
            start(lat_plane(p))
            wait(lat_plane(p))
            merge(range(3), z)

            @pl.when(jnp.logical_or(even, p >= 4))
            def _():
                first(z - 1)

            @pl.when(jnp.logical_or(even, p >= 6))
            def _():
                second(z - 2)

        lax.fori_loop(2, cz, plane, None)

        @pl.when(jnp.logical_not(even))
        def _():
            head_chem.wait_recv()
            head_phi.wait_recv()
            start(lat_head)

            @pl.when(gets_end)
            def _():
                end_chem.wait_recv()
                end_phi.wait_recv()
                start(lat_end)

            wait(lat_head)
            for z in (2, 3):
                merge(range(5), z)
            firsts(1, 5)
            seconds(2, 6)

        @pl.when(gets_end)
        def _():
            wait(lat_end)
            for z in (cz + 2, cz + 3):
                merge(range(5), z)
            firsts(cz + 1, cz + 3)

        @pl.when(jnp.logical_not(gets_end))
        def _():
            for f in range(5):
                g[f, cz + 2] = g[f, cz + 1]
            first(cz + 1)
            for f in range(5):
                half[f, cz + 2] = half[f, cz + 1]

        seconds(cz, cz + 2)

    @pl.when(jnp.logical_not(gets))
    def _():
        def entering(o, _):
            kind = index[o]
            for a in range(4):
                staged[a, o] = jnp.full((nx, ny), 1.0 if a == 0 else 0.0, jnp.float32)
            for k in range(2):
                value = jnp.zeros((nx, ny), jnp.float32)
                for liquid in range(table.shape[1]):
                    value = jnp.where(kind == liquid, table[k, liquid], value)
                staged[4 + k, o] = value
            start(put(o))
            return _

        lax.fori_loop(0, cz, entering, None)

    @pl.when(gives_end)
    def _():
        end_chem.wait_send()
        end_phi.wait_send()

    @pl.when(odd_gives)
    def _():
        head_chem.wait_send()
        head_phi.wait_send()

    @pl.when(gives)
    def _():
        body_chem.wait_send()

        def gone(p, _):
            plane_phi(p).wait_send()
            return _

        lax.fori_loop(2, cz, gone, None)

    @pl.when(jnp.logical_and(even, gets_end))
    def _():
        pass_chem.wait_send()
        pass_phi.wait_send()

    def written(o, _):
        wait(put(o))
        return _

    lax.fori_loop(0, cz, written, None)


def body(labels, seed_blend, potential, inflow_index, liquid_table):
    n, m = lax.axis_size("grow"), lax.axis_size("lat")
    cz, nx, ny = labels.shape
    anywhere = pl.BlockSpec(memory_space=pl.ANY)
    dma = pltpu.SemaphoreType.DMA
    f32 = jnp.float32
    return pl.pallas_call(
        functools.partial(kernel, n, m),
        out_shape=(jax.ShapeDtypeStruct((4, cz, nx, ny), f32), jax.ShapeDtypeStruct((2, cz, nx, ny), f32)),
        in_specs=[pl.BlockSpec(memory_space=pltpu.HBM)] * 5,
        out_specs=(anywhere, anywhere),
        scratch_shapes=[
            pltpu.SMEM(liquid_table.shape[::-1], f32),
            pltpu.VMEM((cz, nx, ny), jnp.int32),
            pltpu.VMEM((4, cz, nx, ny), f32),
            pltpu.VMEM((cz, nx, ny), jnp.int32),
            pltpu.VMEM((3, cz, nx, ny), f32),
            pltpu.VMEM((5, cz + 4, nx + ROWS, ny), f32),
            pltpu.VMEM((5, cz + 4, nx + ROWS, ny), f32),
            pltpu.VMEM((5, cz + 4, ROWS, ny), f32),
            pltpu.VMEM((5, cz + 4, ROWS, ny), f32),
            pltpu.VMEM((6, cz, nx, ny), f32),
            dma((5,)),
            dma((7,)),
            dma((cz,)),
            dma((5,)),
            dma((cz,)),
            dma((2, 4 + cz)),
            dma((2, 4 + cz)),
            dma((2, cz)),
        ],
        compiler_params=pltpu.CompilerParams(collective_id=0, has_side_effects=True, vmem_limit_bytes=12 << 20),
    )(*(pltpu.with_memory_space_constraint(a, pltpu.HBM) for a in (labels, seed_blend, potential, inflow_index, liquid_table.T)))


def solution(mesh):
    in_specs = (
        P("grow", "lat", None),
        P(None, "grow", "lat", None),
        P(None, "grow", "lat", None),
        P(None, "lat", None),
        P(),
    )
    out_specs = (P(None, "grow", "lat", None), P(None, "grow", "lat", None))
    return jax.shard_map(body, mesh=mesh, in_specs=in_specs, out_specs=out_specs, check_vma=False)
```

```python
import functools

import jax
import jax.numpy as jnp
from jax import lax
from jax.experimental import pallas as pl
from jax.experimental.pallas import tpu as pltpu
from jax.sharding import PartitionSpec as P

offset_table = ((0.0, 0.0), (0.6, -0.3), (-0.4, 0.5), (-0.2, -0.6))
latent_heat = (0.0, 0.8, 0.8, 0.8)
relax_rate = 0.1
diffusion = 0.05
MESH = pl.DeviceIdType.MESH
ROWS = 8


def advance(phi, chem, lap, temp):
    phi = list(phi) + [1.0 - (phi[0] + phi[1] + phi[2])]
    square = chem[0] * chem[0] + chem[1] * chem[1]
    pull = []
    for a in range(4):
        e0, e1 = offset_table[a]
        p = phi[a]
        w = square - (1.0 - p) * (1.0 - 2.0 * p)
        if a:
            w = w + ((2.0 * e0) * chem[0] + (2.0 * e1) * chem[1] + ((e0 * e0 + e1 * e1) - 2.0 * latent_heat[a] * temp))
        pull.append(p * w)
    mean = 0.25 * ((pull[0] + pull[1]) + (pull[2] + pull[3]))
    new = [phi[a] + relax_rate * ((lap[a] + pull[a]) - mean) for a in range(3)]
    new.append(1.0 - (new[0] + new[1] + new[2]))
    squares = [v * v for v in new]
    growth = [squares[a] - phi[a] * phi[a] for a in range(4)]
    total = (growth[0] + growth[1]) + (growth[2] + growth[3])
    inverse = 1.0 / ((squares[0] + squares[1]) + (squares[2] + squares[3]))
    mobile = diffusion * (0.1 + squares[0])
    out = []
    for k in range(2):
        source = chem[k] * total
        for a in range(1, 4):
            source = source + offset_table[a][k] * growth[a]
        out.append(chem[k] + (mobile * lap[3 + k] - source) * inverse)
    return new, out


def kernel(n, m, labels_h, blend_h, chem_h, index_h, table_h, staged,
           table, labels, blend, index, own, g, half, from_right, from_left, relay,
           load_sem, send_sem, plane_send, recv_sem, plane_recv, lat_send, lat_recv):
    cz, nx, ny = labels.shape
    tiles = nx // ROWS
    me = lax.axis_index("grow")
    lat = lax.axis_index("lat")
    right, left = lax.rem(lat + 1, m), lax.rem(lat + m - 1, m)
    even = lax.rem(me, 2) == 0
    corner = lax.rem(me, 4)
    gives, gives_end = me > 0, jnp.logical_and(me > 1, corner != 0)
    gives_via, gets_via = jnp.logical_and(me > 1, corner == 0), jnp.logical_and(me > 4, corner == 2)
    gets, gets_end = me < n - 1, me < n - 2
    row = lax.broadcasted_iota(jnp.int32, (ROWS, ny), 0)

    loads = [
        pltpu.make_async_copy(labels_h, labels, load_sem.at[0]),
        pltpu.make_async_copy(blend_h, blend, load_sem.at[1]),
        pltpu.make_async_copy(index_h, index, load_sem.at[2]),
        pltpu.make_async_copy(chem_h.at[:, cz - 2 : cz], g.at[3:5, 0:2, 0:nx], load_sem.at[3]),
        pltpu.make_async_copy(table_h, table, load_sem.at[4]),
    ]
    for load in loads:
        load.start()

    barrier = pltpu.get_barrier_semaphore()
    met = jnp.int32(2)
    for step in (-2, -1, 1, 2):
        there = jnp.logical_and(me + step >= 0, me + step < n)
        met = met + there.astype(jnp.int32)

        @pl.when(there)
        def _():
            pl.semaphore_signal(barrier, inc=1, device_id={"grow": me + step}, device_id_type=MESH)

    for step in (-4, 4):
        there = jnp.logical_and(corner == 2, jnp.logical_and(me + step > 0, me + step < n))
        met = met + there.astype(jnp.int32)

        @pl.when(there)
        def _():
            pl.semaphore_signal(barrier, inc=1, device_id={"grow": me + step}, device_id_type=MESH)

    for side in (left, right):
        pl.semaphore_signal(barrier, inc=1, device_id={"lat": side}, device_id_type=MESH)
    pl.semaphore_wait(barrier, met)

    below, below2 = lax.rem(me + n - 1, n), lax.rem(me + 2 * n - 2, n)
    above, above2, below4 = lax.rem(me + 1, n), lax.rem(me + 2, n), lax.rem(me + n - 4, n)

    def along(src, dst, send, recv, device):
        return pltpu.make_async_remote_copy(
            src_ref=src, dst_ref=dst, send_sem=send, recv_sem=recv,
            device_id={"grow": device}, device_id_type=MESH)

    end_chem = along(chem_h.at[:, 0:2], g.at[3:5, cz + 2 : cz + 4, 0:nx], send_sem.at[0], recv_sem.at[0], below2)
    end_phi = along(own.at[:, 0:2], g.at[0:3, cz + 2 : cz + 4, 0:nx], send_sem.at[1], recv_sem.at[1], below2)
    head_chem = along(chem_h.at[:, 0:2], g.at[3:5, 2:4, 0:nx], send_sem.at[2], recv_sem.at[2], below)
    head_phi = along(own.at[:, 0:2], g.at[0:3, 2:4, 0:nx], send_sem.at[3], recv_sem.at[3], below)
    body_chem = along(chem_h.at[:, 2:cz], g.at[3:5, 4 : cz + 2, 0:nx], send_sem.at[4], recv_sem.at[4], below)
    pass_chem = along(g.at[3:5, cz + 2 : cz + 4, 0:nx], g.at[3:5, 2:4, 0:nx], send_sem.at[5], recv_sem.at[2], above)
    pass_phi = along(g.at[0:3, cz + 2 : cz + 4, 0:nx], g.at[0:3, 2:4, 0:nx], send_sem.at[6], recv_sem.at[3], above)

    via_chem = along(chem_h.at[:, 0:2], relay.at[3:5], send_sem.at[0], recv_sem.at[5], above2)
    via_phi = along(own.at[:, 0:2], relay.at[0:3], send_sem.at[1], recv_sem.at[6], above2)
    far_chem = along(relay.at[3:5], g.at[3:5, cz + 2 : cz + 4, 0:nx], send_sem.at[7], recv_sem.at[0], below4)
    far_phi = along(relay.at[0:3], g.at[0:3, cz + 2 : cz + 4, 0:nx], send_sem.at[8], recv_sem.at[1], below4)

    def plane_phi(p):
        return along(own.at[:, pl.ds(p, 1)], g.at[0:3, pl.ds(p + 2, 1), 0:nx], plane_send.at[p], plane_recv.at[p], below)

    odd_gives = jnp.logical_and(gives, jnp.logical_not(even))

    @pl.when(gives_end)
    def _():
        end_chem.start()

    @pl.when(gives_via)
    def _():
        via_chem.start()

    @pl.when(odd_gives)
    def _():
        head_chem.start()

    @pl.when(gives)
    def _():
        body_chem.start()

    loads[0].wait()
    loads[1].wait()

    def initial(p, _):
        kind = labels[p]
        weights = [blend[a, p] for a in range(4)]
        inverse = 1.0 / (1.0 + ((weights[0] + weights[1]) + (weights[2] + weights[3])))
        for a in range(3):
            own[a, p] = (jnp.where(kind == a, 1.0, 0.0) + weights[a]) * inverse
        return _

    lax.fori_loop(0, cz, initial, None)
    for k in range(2):
        for a in range(3):
            g[a, k, 0:nx] = own[a, cz - 2 + k]

    @pl.when(gives_end)
    def _():
        end_phi.start()

    @pl.when(gives_via)
    def _():
        via_phi.start()

    @pl.when(odd_gives)
    def _():
        head_phi.start()

    @pl.when(gives)
    def _():
        def go(p, _):
            plane_phi(p).start()
            return _

        lax.fori_loop(2, cz, go, None)

    loads[2].wait()
    loads[3].wait()
    loads[4].wait()

    @pl.when(gets_via)
    def _():
        via_chem.wait_recv()
        far_chem.start()
        via_phi.wait_recv()
        far_phi.start()

    def sideways(fields, planes, group):
        return (
            pltpu.make_async_remote_copy(
                src_ref=g.at[fields, planes, nx - ROWS : nx], dst_ref=from_left.at[fields, planes],
                send_sem=lat_send.at[0, group], recv_sem=lat_recv.at[0, group],
                device_id={"lat": right}, device_id_type=MESH),
            pltpu.make_async_remote_copy(
                src_ref=g.at[fields, planes, 0:ROWS], dst_ref=from_right.at[fields, planes],
                send_sem=lat_send.at[1, group], recv_sem=lat_recv.at[1, group],
                device_id={"lat": left}, device_id_type=MESH),
        )

    everything, phases, chemical = slice(0, 5), slice(0, 3), slice(3, 5)
    lat_own = sideways(everything, slice(0, 2), 0)
    lat_head = sideways(everything, slice(2, 4), 1)
    lat_end = sideways(everything, slice(cz + 2, cz + 4), 2)
    lat_chem = sideways(chemical, slice(4, cz + 2), 3)

    def lat_plane(p):
        return sideways(phases, pl.ds(p + 2, 1), 4 + p)

    def start(pair):
        for copy in pair:
            copy.start()

    def wait(pair):
        for copy in pair:
            copy.wait()

    def merge(fields, z):
        for f in fields:
            g[f, z, nx : nx + ROWS] = jnp.where(row < 4, from_right[f, z], from_left[f, z])

    def tile_step(src, z, t):
        def part(f, z, t):
            return src[f, z, t * ROWS : (t + 1) * ROWS]

        after, before = (t + 1) % (tiles + 1), (t + tiles) % (tiles + 1)
        centre, lap = [], []
        for f in range(5):
            c = part(f, z, t)
            up = pltpu.roll(jnp.where(row == 0, part(f, z, after), c), ROWS - 1, 0)
            down = pltpu.roll(jnp.where(row == ROWS - 1, part(f, z, before), c), 1, 0)
            lap.append(
                ((part(f, z + 1, t) + part(f, z - 1, t)) + (up + down))
                + (pltpu.roll(c, ny - 1, 1) + pltpu.roll(c, 1, 1)) - 6.0 * c)
            centre.append(c)
        plane = ((me + 1) * cz - 2 + z).astype(jnp.float32)
        temp = 2.0 * (plane + 0.5) / float(n * cz) - 1.0
        return advance(centre[:3], centre[3:], lap, temp)

    def first(z):
        for t in range(tiles + 1):
            new, chem = tile_step(g, z, t)
            for f, value in enumerate(new[:3] + chem):
                half[f, z, t * ROWS : (t + 1) * ROWS] = value

    def second(z):
        for t in range(tiles):
            new, chem = tile_step(half, z, t)
            for f, value in enumerate(new + chem):
                staged[f, z - 2, t * ROWS : (t + 1) * ROWS] = value

    def firsts(low, high):
        lax.fori_loop(low, high, lambda z, _: first(z), None)

    def seconds(low, high):
        lax.fori_loop(low, high, lambda z, _: second(z), None)

    @pl.when(gets)
    def _():
        start(lat_own)

        @pl.when(jnp.logical_and(even, gets_end))
        def _():
            end_chem.wait_recv()
            pass_chem.start()
            end_phi.wait_recv()
            pass_phi.start()
            start(lat_end)

        @pl.when(even)
        def _():
            head_chem.wait_recv()
            head_phi.wait_recv()
            start(lat_head)

        body_chem.wait_recv()
        start(lat_chem)
        wait(lat_own)
        for z in (0, 1):
            merge(range(5), z)

        @pl.when(even)
        def _():
            wait(lat_head)
            for z in (2, 3):
                merge(range(5), z)
            firsts(1, 3)

        wait(lat_chem)
        lax.fori_loop(4, cz + 2, lambda z, _: merge((3, 4), z), None)

        def plane(p, _):
            z = p + 2
            plane_phi(p).wait_recv()
            start(lat_plane(p))
            wait(lat_plane(p))
            merge(range(3), z)

            @pl.when(jnp.logical_or(even, p >= 4))
            def _():
                first(z - 1)

            @pl.when(jnp.logical_or(even, p >= 6))
            def _():
                second(z - 2)

        lax.fori_loop(2, cz, plane, None)

        @pl.when(jnp.logical_not(even))
        def _():
            head_chem.wait_recv()
            head_phi.wait_recv()
            start(lat_head)

            @pl.when(gets_end)
            def _():
                end_chem.wait_recv()
                end_phi.wait_recv()
                start(lat_end)

            wait(lat_head)
            for z in (2, 3):
                merge(range(5), z)
            firsts(1, 5)
            seconds(2, 6)

        @pl.when(gets_end)
        def _():
            wait(lat_end)
            for z in (cz + 2, cz + 3):
                merge(range(5), z)
            firsts(cz + 1, cz + 3)

        @pl.when(jnp.logical_not(gets_end))
        def _():
            for f in range(5):
                g[f, cz + 2] = g[f, cz + 1]
            first(cz + 1)
            for f in range(5):
                half[f, cz + 2] = half[f, cz + 1]

        seconds(cz, cz + 2)

    @pl.when(jnp.logical_not(gets))
    def _():
        def entering(o, _):
            kind = index[o]
            for a in range(4):
                staged[a, o] = jnp.full((nx, ny), 1.0 if a == 0 else 0.0, jnp.float32)
            for k in range(2):
                value = jnp.zeros((nx, ny), jnp.float32)
                for liquid in range(table.shape[1]):
                    value = jnp.where(kind == liquid, table[k, liquid], value)
                staged[4 + k, o] = value
            return _

        lax.fori_loop(0, cz, entering, None)

    @pl.when(gives_end)
    def _():
        end_chem.wait_send()
        end_phi.wait_send()

    @pl.when(gives_via)
    def _():
        via_chem.wait_send()
        via_phi.wait_send()

    @pl.when(gets_via)
    def _():
        far_chem.wait_send()
        far_phi.wait_send()

    @pl.when(odd_gives)
    def _():
        head_chem.wait_send()
        head_phi.wait_send()

    @pl.when(gives)
    def _():
        body_chem.wait_send()

        def gone(p, _):
            plane_phi(p).wait_send()
            return _

        lax.fori_loop(2, cz, gone, None)

    @pl.when(jnp.logical_and(even, gets_end))
    def _():
        pass_chem.wait_send()
        pass_phi.wait_send()


def flush(staged, phase_out, chem_out, sem):
    copies = (
        pltpu.make_async_copy(staged.at[0:4], phase_out, sem.at[0]),
        pltpu.make_async_copy(staged.at[4:6], chem_out, sem.at[1]),
    )
    for copy in copies:
        copy.start()
    for copy in copies:
        copy.wait()


def body(labels, seed_blend, potential, inflow_index, liquid_table):
    n, m = lax.axis_size("grow"), lax.axis_size("lat")
    cz, nx, ny = labels.shape
    dma = pltpu.SemaphoreType.DMA
    f32 = jnp.float32
    vmem, hbm = pl.BlockSpec(memory_space=pltpu.VMEM), pl.BlockSpec(memory_space=pltpu.HBM)
    staged = pl.pallas_call(
        functools.partial(kernel, n, m),
        out_shape=pltpu.VMEM((6, cz, nx, ny), f32),
        in_specs=[hbm] * 5,
        out_specs=vmem,
        scratch_shapes=[
            pltpu.SMEM(liquid_table.shape[::-1], f32),
            pltpu.VMEM((cz, nx, ny), jnp.int32),
            pltpu.VMEM((4, cz, nx, ny), f32),
            pltpu.VMEM((cz, nx, ny), jnp.int32),
            pltpu.VMEM((3, cz, nx, ny), f32),
            pltpu.VMEM((5, cz + 4, nx + ROWS, ny), f32),
            pltpu.VMEM((5, cz + 4, nx + ROWS, ny), f32),
            pltpu.VMEM((5, cz + 4, ROWS, ny), f32),
            pltpu.VMEM((5, cz + 4, ROWS, ny), f32),
            pltpu.VMEM((5, 2, nx, ny), f32),
            dma((5,)),
            dma((9,)),
            dma((cz,)),
            dma((7,)),
            dma((cz,)),
            dma((2, 4 + cz)),
            dma((2, 4 + cz)),
        ],
        compiler_params=pltpu.CompilerParams(collective_id=0, has_side_effects=True, vmem_limit_bytes=12 << 20),
    )(*(pltpu.with_memory_space_constraint(a, pltpu.HBM) for a in (labels, seed_blend, potential, inflow_index, liquid_table.T)))
    return pl.pallas_call(
        flush,
        out_shape=(jax.ShapeDtypeStruct((4, cz, nx, ny), f32), jax.ShapeDtypeStruct((2, cz, nx, ny), f32)),
        in_specs=[pl.BlockSpec(memory_space=pl.ANY)],
        out_specs=(hbm, hbm),
        scratch_shapes=[dma((2,))],
        compiler_params=pltpu.CompilerParams(vmem_limit_bytes=1 << 20),
    )(pltpu.with_memory_space_constraint(staged, pltpu.VMEM))


def solution(mesh):
    in_specs = (
        P("grow", "lat", None),
        P(None, "grow", "lat", None),
        P(None, "grow", "lat", None),
        P(None, "lat", None),
        P(),
    )
    out_specs = (P(None, "grow", "lat", None), P(None, "grow", "lat", None))
    return jax.shard_map(body, mesh=mesh, in_specs=in_specs, out_specs=out_specs, check_vma=False)
```

```python
import functools

import jax
import jax.numpy as jnp
from jax import lax
from jax.experimental import pallas as pl
from jax.experimental.pallas import tpu as pltpu
from jax.sharding import PartitionSpec as P

offset_table = ((0.0, 0.0), (0.6, -0.3), (-0.4, 0.5), (-0.2, -0.6))
latent_heat = (0.0, 0.8, 0.8, 0.8)
relax_rate = 0.1
diffusion = 0.05
MESH = pl.DeviceIdType.MESH
ROWS = 8


def advance(phi, chem, lap, temp):
    phi = list(phi) + [1.0 - (phi[0] + phi[1] + phi[2])]
    square = chem[0] * chem[0] + chem[1] * chem[1]
    pull = []
    for a in range(4):
        e0, e1 = offset_table[a]
        p = phi[a]
        w = square - (1.0 - p) * (1.0 - 2.0 * p)
        if a:
            w = w + ((2.0 * e0) * chem[0] + (2.0 * e1) * chem[1] + ((e0 * e0 + e1 * e1) - 2.0 * latent_heat[a] * temp))
        pull.append(p * w)
    mean = 0.25 * ((pull[0] + pull[1]) + (pull[2] + pull[3]))
    new = [phi[a] + relax_rate * ((lap[a] + pull[a]) - mean) for a in range(3)]
    new.append(1.0 - (new[0] + new[1] + new[2]))
    squares = [v * v for v in new]
    growth = [squares[a] - phi[a] * phi[a] for a in range(4)]
    total = (growth[0] + growth[1]) + (growth[2] + growth[3])
    inverse = 1.0 / ((squares[0] + squares[1]) + (squares[2] + squares[3]))
    mobile = diffusion * (0.1 + squares[0])
    out = []
    for k in range(2):
        source = chem[k] * total
        for a in range(1, 4):
            source = source + offset_table[a][k] * growth[a]
        out.append(chem[k] + (mobile * lap[3 + k] - source) * inverse)
    return new, out


BASE = 32
PLANE, EDGES, MID, LAST, HEAD, PASS_MID, PASS_LAST, END, END_NEXT = range(1, 10)


def schedule(kind, cz):
    pair, head, top = cz - 2, cz - 1, cz + 2
    none = (0, 0)

    def step(event, sent=None, landed=None, halo=none, own=none, two=none):
        return (event, 0 if sent is None else sent + 1, 0 if landed is None else landed + 1, halo, own, two)

    if kind == 0:
        return [
            step(PLANE, 0, cz),
            step(PLANE, 1, 0, none, (1, 1)),
            step(PLANE, 2, 1, (2, 1), (2, 1)),
            *(step(PLANE, p, p - 1, (p, 1), (p, 1), (p - 1, 1)) for p in range(3, pair)),
            step(EDGES, pair, pair - 1, (pair, 1), (pair, 1), (pair - 1, 1)),
            step(0, None, pair, (pair + 1, 3)),
            step(MID, None, None, none, (pair + 1, 1), (pair, 1)),
            step(LAST, None, None, none, (cz, 3), (cz - 1, 3)),
        ]
    body = [step(PLANE, 2), step(PLANE, 3, 2)]
    if kind == 1:
        return [
            *body,
            step(PLANE, 4, 3),
            step(PLANE, 5, 4, (5, 1), (5, 1)),
            *(step(PLANE, p, p - 1, (p, 1), (p, 1), (p - 1, 1) if p > 6 else none) for p in range(6, pair)),
            step(EDGES, pair, pair - 1, (pair, 1), (pair, 1), (pair - 1, 1) if pair > 6 else none),
            step(0, None, pair, (pair + 1, 2)),
            step(MID, None, None, none, (pair + 1, 1), (pair, 1)),
            step(LAST, None, None, none, (cz, 1), (cz - 1, 1)),
            step(HEAD, head),
            step(0, None, head, (2, 3)),
            step(PASS_MID, None, None, none, (4, 1), (5, 1)),
            step(PASS_LAST, None, None, none, (1, 3), (2, 3)),
            step(END, cz),
            step(0, None, cz, (cz + 1, 1), (cz + 1, 1), (cz, 1)),
            step(END_NEXT, None, None, none, (top, 1), (cz + 1, 1)),
        ]
    return [
        *body,
        step(END, cz, 3),
        step(PLANE, 4, cz),
        step(END_NEXT, None, 4, (5, 1), (5, 1)),
        step(PLANE, 5),
        *(step(PLANE, p, p - 1, (p, 1), (p, 1), (p - 1, 1) if p > 6 else none) for p in range(6, pair)),
        step(HEAD, head, pair - 1, (pair, 1), (pair, 1), (pair - 1, 1) if pair > 6 else none),
        step(EDGES, pair, head, (2, 3)),
        step(PASS_MID, None, None, none, (4, 1), (5, 1)),
        step(PASS_LAST, None, None, none, (1, 3), (2, 3)),
        step(MID, None, pair, (pair + 1, 3), (pair + 1, 1), (pair, 1)),
        step(LAST, None, None, none, (cz, 3), (cz - 1, 3)),
    ]


def pack(step):
    event, sent, landed, halo, own, two = step
    work = 0
    for low, number in (two, own, halo):
        work = work * (4 * BASE) + low + BASE * number
    return event + BASE * (sent + BASE * landed), work


def kernel(n, m, labels_h, blend_h, chem_h, index_h, table_h, staged,
           table, labels, blend, index, own, g, half, from_right, from_left, relay,
           load_sem, send_sem, recv_sem, plane_send, plane_recv, lat_send, lat_recv, go):
    cz, nx, ny = labels.shape
    tiles = nx // ROWS
    inner = tuple(range(tiles))
    top = cz + 2
    me = lax.axis_index("grow")
    lat = lax.axis_index("lat")
    right, left = lax.rem(lat + 1, m), lax.rem(lat + m - 1, m)
    corner = lax.rem(me, 4)
    even = lax.rem(me, 2) == 0
    odd = jnp.logical_not(even)
    gives, gets = me > 0, me < n - 1
    gets_end = me < n - 2
    gives_via = jnp.logical_and(corner == 0, me > 0)
    gets_via = jnp.logical_and(corner == 2, me > 4)
    row = lax.broadcasted_iota(jnp.int32, (ROWS, ny), 0)

    barrier = pltpu.get_barrier_semaphore()

    def greet(there, device):
        @pl.when(there)
        def _():
            pl.semaphore_signal(barrier, inc=1, device_id={"grow": device}, device_id_type=MESH)

    greet(odd, me - 1)
    greet(even, me + 1)
    greet(jnp.logical_and(odd, me + 1 < n), me + 1)
    greet(corner == 0, me + 2)
    greet(gets_via, me - 2)
    greet(jnp.logical_and(corner == 2, me + 4 < n), me + 4)
    for side in (left, right):
        pl.semaphore_signal(barrier, inc=1, device_id={"lat": side}, device_id_type=MESH)

    loads = [
        pltpu.make_async_copy(labels_h, labels, load_sem.at[0]),
        pltpu.make_async_copy(blend_h, blend, load_sem.at[1]),
        pltpu.make_async_copy(index_h, index, load_sem.at[2]),
        pltpu.make_async_copy(chem_h.at[:, cz - 2 : cz], g.at[3:5, 0:2, 0:nx], load_sem.at[3]),
        pltpu.make_async_copy(table_h, table, load_sem.at[4]),
    ]
    for load in loads:
        load.start()

    met = 3 + jnp.where(even, (me > 0).astype(jnp.int32) + (corner == 2).astype(jnp.int32)
                        + gets_via.astype(jnp.int32) + gives_via.astype(jnp.int32), 0)
    pl.semaphore_wait(barrier, met)

    @pl.when(even)
    def _():
        pl.semaphore_signal(go, inc=1, device_id={"grow": me + 1}, device_id_type=MESH)

    def to(step):
        return lax.rem(me + n + step, n)

    def along(src, dst, send, recv, device):
        return pltpu.make_async_remote_copy(
            src_ref=src, dst_ref=dst, send_sem=send_sem.at[send], recv_sem=recv_sem.at[recv],
            device_id={"grow": device}, device_id_type=MESH)

    low, middle, high = pl.ds(0, ROWS), pl.ds(ROWS, nx - 2 * ROWS), pl.ds(nx - ROWS, ROWS)
    rows = pl.ds(0, nx)

    end = (
        along(chem_h.at[:, 0:2], g.at[3:5, top : top + 2, rows], 0, 0, to(-2)),
        along(own.at[:, 0:1], g.at[0:3, top : top + 1, rows], 1, 1, to(-2)),
        along(own.at[:, 1:2], g.at[0:3, top + 1 : top + 2, rows], 2, 2, to(-2)),
    )
    via = (
        along(chem_h.at[:, 0:2], relay.at[3:5], 0, 13, to(2)),
        along(own.at[:, 0:1], relay.at[0:3, 0:1], 1, 14, to(2)),
        along(own.at[:, 1:2], relay.at[0:3, 1:2], 2, 15, to(2)),
    )
    far = (
        along(relay.at[3:5], g.at[3:5, top : top + 2, rows], 13, 0, to(-4)),
        along(relay.at[0:3, 0:1], g.at[0:3, top : top + 1, rows], 14, 1, to(-4)),
        along(relay.at[0:3, 1:2], g.at[0:3, top + 1 : top + 2, rows], 15, 2, to(-4)),
    )
    head_chem = along(chem_h.at[:, 0:2], g.at[3:5, 2:4, rows], 3, 3, to(-1))
    lead_chem = along(chem_h.at[:, 2:4], g.at[3:5, 4:6, rows], 16, 16, to(-1))
    body_chem = along(chem_h.at[:, 4:cz], g.at[3:5, 6:top, rows], 4, 4, to(-1))
    def banded(src, dst, send, recv, device):
        return [
            along(src(planes, band), dst(planes, band), send + k, recv + k, device)
            for k, (planes, band) in enumerate(
                ((pl.ds(0, 2), low), (pl.ds(0, 2), high), (pl.ds(0, 1), middle), (pl.ds(1, 1), middle)))
        ]

    final_own, final_g = own.at[:, cz - 2 : cz], g.at[0:3, cz:top]
    last_phi = banded(lambda p, r: final_own.at[:, p, r], lambda p, r: final_g.at[:, p, r], 5, 5, to(-1))
    end_g, head_g = g.at[0:3, top : top + 2], g.at[0:3, 2:4]
    pass_chem = along(g.at[3:5, top : top + 2, rows], g.at[3:5, 2:4, rows], 17, 3, to(1))
    pass_phi = banded(lambda p, r: end_g.at[:, p, r], lambda p, r: head_g.at[:, p, r], 9, 9, to(1))
    pass_phi = [pass_phi[0], pass_phi[1], pass_phi[3], pass_phi[2]]

    def plane_phi(p):
        return pltpu.make_async_remote_copy(
            src_ref=own.at[:, pl.ds(p, 1)], dst_ref=g.at[0:3, pl.ds(p + 2, 1), rows],
            send_sem=plane_send.at[p], recv_sem=plane_recv.at[p],
            device_id={"grow": to(-1)}, device_id_type=MESH)

    gives_end = jnp.logical_and(me > 1, corner != 0)
    even_end = jnp.logical_and(corner == 2, me > 1)
    odd_end = jnp.logical_and(odd, me > 1)

    @pl.when(odd)
    def _():
        head_chem.start()

    @pl.when(gives)
    def _():
        lead_chem.start()
        body_chem.start()

    @pl.when(even_end)
    def _():
        end[0].start()

    @pl.when(gives_via)
    def _():
        via[0].start()

    loads[0].wait()
    loads[1].wait()

    def initial(p, _):
        kind = labels[p]
        weights = [blend[a, p] for a in range(4)]
        inverse = 1.0 / (1.0 + ((weights[0] + weights[1]) + (weights[2] + weights[3])))
        for a in range(3):
            own[a, p] = (jnp.where(kind == a, 1.0, 0.0) + weights[a]) * inverse
        return _

    lax.fori_loop(0, cz, initial, None)

    @pl.when(odd)
    def _():
        plane_phi(0).start()
        plane_phi(1).start()

    @pl.when(even_end)
    def _():
        end[1].start()
        end[2].start()

    @pl.when(gives_via)
    def _():
        via[1].start()
        via[2].start()

    def planes(low_p, high_p, act):
        def step(p, _):
            act(plane_phi(p))
            return _

        lax.fori_loop(low_p, high_p, step, None)

    @pl.when(gives)
    def _():
        planes(2, cz - 2, lambda copy: copy.start())
        for copy in last_phi:
            copy.start()

    for k in range(2):
        for a in range(3):
            g[a, k, 0:nx] = own[a, cz - 2 + k]

    @pl.when(odd)
    def _():
        pl.semaphore_wait(go, 1)

    loads[2].wait()
    loads[3].wait()
    loads[4].wait()

    @pl.when(gets_via)
    def _():
        for landed, onward in zip(via, far):
            landed.wait_recv()
            onward.start()

    def sideways(fields, planes, group):
        return (
            pltpu.make_async_remote_copy(
                src_ref=g.at[fields, planes, nx - ROWS : nx], dst_ref=from_left.at[fields, planes],
                send_sem=lat_send.at[0, group], recv_sem=lat_recv.at[0, group],
                device_id={"lat": right}, device_id_type=MESH),
            pltpu.make_async_remote_copy(
                src_ref=g.at[fields, planes, 0:ROWS], dst_ref=from_right.at[fields, planes],
                send_sem=lat_send.at[1, group], recv_sem=lat_recv.at[1, group],
                device_id={"lat": left}, device_id_type=MESH),
        )

    everything, phases, chemical = slice(0, 5), slice(0, 3), slice(3, 5)
    lat_own = sideways(everything, slice(1, 2), 0)
    lat_head_chem = sideways(chemical, slice(2, 4), 1)
    lat_end_chem = sideways(chemical, slice(top, top + 1), 2)
    lat_chem = sideways(chemical, slice(4, top), 3)

    lat_pair = sideways(phases, slice(cz, top), 4 + cz - 2)
    lat_head = sideways(phases, slice(2, 4), 4 + cz - 1)

    def lat_plane(p):
        return sideways(phases, pl.ds(p + 2, 1), 4 + p)

    def start(pair):
        for copy in pair:
            copy.start()

    def wait(pair):
        for copy in pair:
            copy.wait()

    def merge(fields, z):
        for f in fields:
            g[f, z, nx : nx + ROWS] = jnp.where(row < 4, from_right[f, z], from_left[f, z])

    def tile_step(src, z, t):
        def part(f, z, t):
            return src[f, z, t * ROWS : (t + 1) * ROWS]

        after, before = (t + 1) % (tiles + 1), (t + tiles) % (tiles + 1)
        centre, lap = [], []
        for f in range(5):
            c = part(f, z, t)
            up = pltpu.roll(jnp.where(row == 0, part(f, z, after), c), ROWS - 1, 0)
            down = pltpu.roll(jnp.where(row == ROWS - 1, part(f, z, before), c), 1, 0)
            lap.append(
                ((part(f, z + 1, t) + part(f, z - 1, t)) + (up + down))
                + (pltpu.roll(c, ny - 1, 1) + pltpu.roll(c, 1, 1)) - 6.0 * c)
            centre.append(c)
        plane = ((me + 1) * cz - 2 + z).astype(jnp.float32)
        temp = 2.0 * (plane + 0.5) / float(n * cz) - 1.0
        return advance(centre[:3], centre[3:], lap, temp)

    def first(z, parts):
        for t in parts:
            new, chem = tile_step(g, z, t)
            for f, value in enumerate(new[:3] + chem):
                half[f, z, t * ROWS : (t + 1) * ROWS] = value

    def second(z):
        for t in inner:
            new, chem = tile_step(half, z, t)
            for f, value in enumerate(new + chem):
                staged[f, z - 2, t * ROWS : (t + 1) * ROWS] = value

    def chem_in():
        start(lat_own)
        body_chem.wait_recv()
        start(lat_chem)
        wait(lat_own)
        merge(range(5), 1)
        wait(lat_chem)
        lax.fori_loop(4, top, lambda z, _: merge((3, 4), z), None)

    def head_chem_lands():
        wait(lat_head_chem)
        lax.fori_loop(2, 4, lambda z, _: merge((3, 4), z), None)

    @pl.when(jnp.logical_and(even, gets_end))
    def _():
        end[0].wait_recv()
        pass_chem.start()
        start(lat_end_chem)
        end[1].wait_recv()
        start(lat_plane(cz))
        end[2].wait_recv()
        for copy in pass_phi:
            copy.start()

    @pl.when(gets)
    def _():
        lead_chem.wait_recv()

    @pl.when(odd_end)
    def _():
        for copy in end:
            copy.start()

    @pl.when(gets)
    def _():
        chem_in()

    @pl.when(jnp.logical_and(gets, even))
    def _():
        head_chem.wait_recv()
        start(lat_head_chem)
        head_chem_lands()

    code = jnp.where(even, 0, jnp.where(corner == 1, 1, 2))
    plans = [schedule(kind, cz) for kind in range(3)]
    longest = max(len(plan) for plan in plans)
    words = []
    for k in range(longest):
        packed = [pack(plan[k]) if k < len(plan) else (0, 0) for plan in plans]
        words.append([jnp.where(code == 0, p0, jnp.where(code == 1, p1, p2)) for p0, p1, p2 in zip(*packed)])
    count = jnp.where(code == 0, len(plans[0]), jnp.where(code == 1, len(plans[1]), len(plans[2])))
    count = jnp.where(gets, count, 0)
    topmost = jnp.logical_not(gets_end)

    def run(k, _):
        comm, work = words[0]
        for q in range(1, longest):
            comm = jnp.where(k == q, words[q][0], comm)
            work = jnp.where(k == q, words[q][1], work)
        event, sent, landed = comm % BASE, comm // BASE % BASE, comm // (BASE * BASE)

        @pl.when(event == PLANE)
        def _():
            plane_phi(sent - 1).wait_recv()

        @pl.when(event == EDGES)
        def _():
            last_phi[0].wait_recv()
            last_phi[1].wait_recv()
            start(lat_pair)

        @pl.when(event == MID)
        def _():
            last_phi[2].wait_recv()

        @pl.when(event == LAST)
        def _():
            last_phi[3].wait_recv()

        @pl.when(event == HEAD)
        def _():
            head_chem.wait_recv()
            start(lat_head_chem)
            pass_phi[0].wait_recv()
            pass_phi[1].wait_recv()
            start(lat_head)

        @pl.when(event == PASS_MID)
        def _():
            pass_phi[2].wait_recv()

        @pl.when(event == PASS_LAST)
        def _():
            pass_phi[3].wait_recv()

        @pl.when(event == END)
        def _():
            end[0].wait_recv()
            start(lat_end_chem)
            end[1].wait_recv()

        @pl.when(event == END_NEXT)
        def _():
            end[2].wait_recv()

        @pl.when(jnp.logical_or(event == PLANE, event == END))
        def _():
            start(lat_plane(sent - 1))

        ending = landed == cz + 1

        @pl.when(jnp.logical_and(ending, gets_end))
        def _():
            wait(lat_end_chem)
            merge((3, 4), top)

        @pl.when(jnp.logical_or(jnp.logical_and(landed > 0, landed < cz - 1), jnp.logical_and(ending, gets_end)))
        def _():
            wait(lat_plane(landed - 1))
            merge(range(3), landed + 1)

        @pl.when(landed == cz - 1)
        def _():
            wait(lat_pair)
            lax.fori_loop(cz, top, lambda z, _: merge(range(3), z), None)

        @pl.when(landed == cz)
        def _():
            head_chem_lands()
            wait(lat_head)
            lax.fori_loop(2, 4, lambda z, _: merge(range(3), z), None)

        @pl.when(jnp.logical_and(topmost, landed == cz - 1))
        def _():
            for f in range(5):
                g[f, top, nx:] = g[f, top - 1, nx:]

        @pl.when(jnp.logical_and(topmost, event == LAST))
        def _():
            for f in range(5):
                g[f, top, 0:nx] = g[f, top - 1, 0:nx]

        def span(value):
            low_z = value % BASE
            return low_z, low_z + value // BASE

        h0, h1 = span(work % (4 * BASE))
        f0, f1 = span(work // (4 * BASE) % (4 * BASE))
        s0, s1 = span(work // (16 * BASE * BASE))
        lax.fori_loop(h0, h1, lambda z, _: first(z, (tiles,)), None)
        lax.fori_loop(f0, jnp.minimum(f1, jnp.where(topmost, top, top + 1)), lambda z, _: first(z, inner), None)

        @pl.when(jnp.logical_and(topmost, event == LAST))
        def _():
            for f in range(5):
                half[f, top, 0:nx] = half[f, top - 1, 0:nx]

        lax.fori_loop(s0, s1, lambda z, _: second(z), None)
        return _

    lax.fori_loop(0, count, run, None)

    @pl.when(jnp.logical_not(gets))
    def _():
        def entering(o, _):
            kind = index[o]
            for a in range(4):
                staged[a, o] = jnp.full((nx, ny), 1.0 if a == 0 else 0.0, jnp.float32)
            for k in range(2):
                value = jnp.zeros((nx, ny), jnp.float32)
                for liquid in range(table.shape[1]):
                    value = jnp.where(kind == liquid, table[k, liquid], value)
                staged[4 + k, o] = value
            return _

        lax.fori_loop(0, cz, entering, None)

    @pl.when(gives_end)
    def _():
        for copy in end:
            copy.wait_send()

    @pl.when(gives_via)
    def _():
        for copy in via:
            copy.wait_send()

    @pl.when(gets_via)
    def _():
        for copy in far:
            copy.wait_send()

    @pl.when(odd)
    def _():
        head_chem.wait_send()
        plane_phi(0).wait_send()
        plane_phi(1).wait_send()

    @pl.when(gives)
    def _():
        lead_chem.wait_send()
        body_chem.wait_send()
        planes(2, cz - 2, lambda copy: copy.wait_send())
        for copy in last_phi:
            copy.wait_send()

    @pl.when(jnp.logical_and(even, gets_end))
    def _():
        pass_chem.wait_send()
        for copy in pass_phi:
            copy.wait_send()


def flush(staged, phase_out, chem_out, sem):
    copies = (
        pltpu.make_async_copy(staged.at[0:4], phase_out, sem.at[0]),
        pltpu.make_async_copy(staged.at[4:6], chem_out, sem.at[1]),
    )
    for copy in copies:
        copy.start()
    for copy in copies:
        copy.wait()


def body(labels, seed_blend, potential, inflow_index, liquid_table):
    n, m = lax.axis_size("grow"), lax.axis_size("lat")
    cz, nx, ny = labels.shape
    dma = pltpu.SemaphoreType.DMA
    f32 = jnp.float32
    vmem, hbm = pl.BlockSpec(memory_space=pltpu.VMEM), pl.BlockSpec(memory_space=pltpu.HBM)
    staged = pl.pallas_call(
        functools.partial(kernel, n, m),
        out_shape=pltpu.VMEM((6, cz, nx, ny), f32),
        in_specs=[hbm] * 5,
        out_specs=vmem,
        scratch_shapes=[
            pltpu.SMEM(liquid_table.shape[::-1], f32),
            pltpu.VMEM((cz, nx, ny), jnp.int32),
            pltpu.VMEM((4, cz, nx, ny), f32),
            pltpu.VMEM((cz, nx, ny), jnp.int32),
            pltpu.VMEM((3, cz, nx, ny), f32),
            pltpu.VMEM((5, cz + 4, nx + ROWS, ny), f32),
            pltpu.VMEM((5, cz + 4, nx + ROWS, ny), f32),
            pltpu.VMEM((5, cz + 4, ROWS, ny), f32),
            pltpu.VMEM((5, cz + 4, ROWS, ny), f32),
            pltpu.VMEM((5, 2, nx, ny), f32),
            dma((5,)),
            dma((18,)),
            dma((17,)),
            dma((cz,)),
            dma((cz,)),
            dma((2, 5 + cz)),
            dma((2, 5 + cz)),
            pltpu.SemaphoreType.REGULAR,
        ],
        compiler_params=pltpu.CompilerParams(collective_id=0, has_side_effects=True, vmem_limit_bytes=12 << 20),
    )(*(pltpu.with_memory_space_constraint(a, pltpu.HBM) for a in (labels, seed_blend, potential, inflow_index, liquid_table.T)))
    return pl.pallas_call(
        flush,
        out_shape=(jax.ShapeDtypeStruct((4, cz, nx, ny), f32), jax.ShapeDtypeStruct((2, cz, nx, ny), f32)),
        in_specs=[pl.BlockSpec(memory_space=pl.ANY)],
        out_specs=(hbm, hbm),
        scratch_shapes=[dma((2,))],
        compiler_params=pltpu.CompilerParams(vmem_limit_bytes=1 << 20),
    )(pltpu.with_memory_space_constraint(staged, pltpu.VMEM))


def solution(mesh):
    in_specs = (
        P("grow", "lat", None),
        P(None, "grow", "lat", None),
        P(None, "grow", "lat", None),
        P(None, "lat", None),
        P(),
    )
    out_specs = (P(None, "grow", "lat", None), P(None, "grow", "lat", None))
    return jax.shard_map(body, mesh=mesh, in_specs=in_specs, out_specs=out_specs, check_vma=False)
```

```python
import functools

import jax
import jax.numpy as jnp
from jax import lax
from jax.experimental import pallas as pl
from jax.experimental.pallas import tpu as pltpu
from jax.sharding import PartitionSpec as P

offset_table = ((0.0, 0.0), (0.6, -0.3), (-0.4, 0.5), (-0.2, -0.6))
latent_heat = (0.0, 0.8, 0.8, 0.8)
relax_rate = 0.1
diffusion = 0.05
MESH = pl.DeviceIdType.MESH
ROWS = 8
LATE = 3


def advance(phi, chem, lap, temp):
    phi = list(phi) + [1.0 - (phi[0] + phi[1] + phi[2])]
    square = chem[0] * chem[0] + chem[1] * chem[1]
    pull = []
    for a in range(4):
        e0, e1 = offset_table[a]
        p = phi[a]
        w = square - (1.0 - p) * (1.0 - 2.0 * p)
        if a:
            w = w + ((2.0 * e0) * chem[0] + (2.0 * e1) * chem[1] + ((e0 * e0 + e1 * e1) - 2.0 * latent_heat[a] * temp))
        pull.append(p * w)
    mean = 0.25 * ((pull[0] + pull[1]) + (pull[2] + pull[3]))
    new = [phi[a] + relax_rate * ((lap[a] + pull[a]) - mean) for a in range(3)]
    new.append(1.0 - (new[0] + new[1] + new[2]))
    squares = [v * v for v in new]
    growth = [squares[a] - phi[a] * phi[a] for a in range(4)]
    total = (growth[0] + growth[1]) + (growth[2] + growth[3])
    inverse = 1.0 / ((squares[0] + squares[1]) + (squares[2] + squares[3]))
    mobile = diffusion * (0.1 + squares[0])
    out = []
    for k in range(2):
        source = chem[k] * total
        for a in range(1, 4):
            source = source + offset_table[a][k] * growth[a]
        out.append(chem[k] + (mobile * lap[3 + k] - source) * inverse)
    return new, out


def tile_step(src, z, t, tiles, plane, planes):
    ny = src.shape[-1]
    row = lax.broadcasted_iota(jnp.int32, (ROWS, ny), 0)

    def part(f, z, t):
        return src[f, z, t * ROWS : (t + 1) * ROWS]

    after, before = (t + 1) % (tiles + 1), (t + tiles) % (tiles + 1)
    centre, lap = [], []
    for f in range(5):
        c = part(f, z, t)
        up = pltpu.roll(jnp.where(row == 0, part(f, z, after), c), ROWS - 1, 0)
        down = pltpu.roll(jnp.where(row == ROWS - 1, part(f, z, before), c), 1, 0)
        lap.append(
            ((part(f, z + 1, t) + part(f, z - 1, t)) + (up + down))
            + (pltpu.roll(c, ny - 1, 1) + pltpu.roll(c, 1, 1)) - 6.0 * c)
        centre.append(c)
    temp = 2.0 * (plane.astype(jnp.float32) + 0.5) / float(planes) - 1.0
    return advance(centre[:3], centre[3:], lap, temp)


PLANE, EDGES, MID, LAST, HEAD, PASS_MID, PASS_LAST, END, END_NEXT = range(1, 10)


def schedule(kind, cz):
    pair, head, top = cz - 2, cz - 1, cz + 2
    none = (0, 0)

    def step(event, sent=None, landed=None, halo=none, own=none, two=none):
        return (event, 0 if sent is None else sent + 1, 0 if landed is None else landed + 1, halo, own, two)

    if kind == 0:
        return [
            step(PLANE, 0, cz),
            step(PLANE, 1, 0, none, (1, 1)),
            step(PLANE, 2, 1, (2, 1), (2, 1)),
            *(step(PLANE, p, p - 1, (p, 1), (p, 1), (p - 1, 1)) for p in range(3, pair)),
            step(EDGES, pair, pair - 1, (pair, 1), (pair, 1), (pair - 1, 1)),
            step(0, None, pair, (pair + 1, 3)),
            step(MID, None, None, none, (pair + 1, 1), (pair, 1)),
            step(LAST, None, None, none, (cz, 3), (cz - 1, 3)),
        ]
    body = [step(PLANE, 2), step(PLANE, 3, 2)]
    if kind == 1:
        return [
            *body,
            step(PLANE, 4, 3),
            step(PLANE, 5, 4, (5, 1), (5, 1)),
            *(step(PLANE, p, p - 1, (p, 1), (p, 1), (p - 1, 1) if p > 6 else none) for p in range(6, pair)),
            step(EDGES, pair, pair - 1, (pair, 1), (pair, 1), (pair - 1, 1) if pair > 6 else none),
            step(0, None, pair, (pair + 1, 2)),
            step(MID, None, None, none, (pair + 1, 1), (pair, 1)),
            step(LAST, None, None, none, (cz, 1), (cz - 1, 1)),
            step(HEAD, head),
            step(0, None, head, (2, 3)),
            step(PASS_MID, None, None, none, (4, 1), (5, 1)),
            step(PASS_LAST, None, None, none, (1, 3), (2, 3)),
            step(END, cz),
            step(0, None, cz, (cz + 1, 1), (cz + 1, 1), (cz, 1)),
            step(END_NEXT, None, None, none, (top, 1), (cz + 1, 1)),
        ]
    return [
        *body,
        step(END, cz, 3),
        step(PLANE, 4, cz),
        step(END_NEXT, None, 4, (5, 1), (5, 1)),
        step(PLANE, 5),
        *(step(PLANE, p, p - 1, (p, 1), (p, 1), (p - 1, 1) if p > 6 else none) for p in range(6, pair)),
        step(HEAD, head, pair - 1, (pair, 1), (pair, 1), (pair - 1, 1) if pair > 6 else none),
        step(PASS_MID, None, head, (2, 3), (4, 1), (5, 1)),
        step(EDGES, pair),
        step(PASS_LAST, None, None, none, (1, 3), (2, 3)),
        step(MID, None, pair, (pair + 1, 3), (pair + 1, 1), (pair, 1)),
        step(LAST, None, None, none, (cz, 3), (cz - 1, 3)),
    ]


BASE = 32


def pack(step):
    event, sent, landed, halo, own, two = step
    work = 0
    for low, number in (two, own, halo):
        work = work * (4 * BASE) + low + BASE * number
    return event + BASE * (sent + BASE * landed), work


def pick(k, values):
    bit = 1
    while len(values) > 1:
        odd = k // bit % 2 == 1
        paired = [jnp.where(odd, b, a) for a, b in zip(values[0::2], values[1::2])]
        values = paired + values[len(values) - len(values) % 2 :]
        bit *= 2
    return values[0]


def kernel(n, m, labels_h, blend_h, chem_h, index_h, table_h, staged, half,
           table, labels, blend, index, own, g, from_right, from_left, relay,
           load_sem, send_sem, recv_sem, plane_send, plane_recv, lat_send, lat_recv, go):
    cz, nx, ny = labels.shape
    tiles = nx // ROWS
    inner = tuple(range(tiles))
    top = cz + 2
    me = lax.axis_index("grow")
    lat = lax.axis_index("lat")
    right, left = lax.rem(lat + 1, m), lax.rem(lat + m - 1, m)
    corner = lax.rem(me, 4)
    even = lax.rem(me, 2) == 0
    odd = jnp.logical_not(even)
    gives, gets = me > 0, me < n - 1
    gets_end = me < n - 2
    gives_via = jnp.logical_and(corner == 0, me > 0)
    gets_via = jnp.logical_and(corner == 2, me > 4)
    row = lax.broadcasted_iota(jnp.int32, (ROWS, ny), 0)

    barrier = pltpu.get_barrier_semaphore()

    def greet(there, device):
        @pl.when(there)
        def _():
            pl.semaphore_signal(barrier, inc=1, device_id={"grow": device}, device_id_type=MESH)

    greet(odd, me - 1)
    greet(even, me + 1)
    greet(jnp.logical_and(odd, me + 1 < n), me + 1)
    greet(corner == 0, me + 2)
    greet(gets_via, me - 2)
    greet(jnp.logical_and(corner == 2, me + 4 < n), me + 4)
    for side in (left, right):
        pl.semaphore_signal(barrier, inc=1, device_id={"lat": side}, device_id_type=MESH)

    loads = [
        pltpu.make_async_copy(labels_h, labels, load_sem.at[0]),
        pltpu.make_async_copy(blend_h, blend, load_sem.at[1]),
        pltpu.make_async_copy(index_h, index, load_sem.at[2]),
        pltpu.make_async_copy(chem_h.at[:, cz - 2 : cz], g.at[3:5, 0:2, 0:nx], load_sem.at[3]),
        pltpu.make_async_copy(table_h, table, load_sem.at[4]),
    ]
    for load in loads:
        load.start()

    met = 3 + jnp.where(even, (me > 0).astype(jnp.int32) + (corner == 2).astype(jnp.int32)
                        + gets_via.astype(jnp.int32) + gives_via.astype(jnp.int32), 0)
    pl.semaphore_wait(barrier, met)

    @pl.when(even)
    def _():
        pl.semaphore_signal(go, inc=1, device_id={"grow": me + 1}, device_id_type=MESH)

    def to(step):
        return lax.rem(me + n + step, n)

    def along(src, dst, send, recv, device):
        return pltpu.make_async_remote_copy(
            src_ref=src, dst_ref=dst, send_sem=send_sem.at[send], recv_sem=recv_sem.at[recv],
            device_id={"grow": device}, device_id_type=MESH)

    low, middle, high = pl.ds(0, ROWS), pl.ds(ROWS, nx - 2 * ROWS), pl.ds(nx - ROWS, ROWS)
    rows = pl.ds(0, nx)

    end = (
        along(chem_h.at[:, 0:2], g.at[3:5, top : top + 2, rows], 0, 0, to(-2)),
        along(own.at[:, 0:1], g.at[0:3, top : top + 1, rows], 1, 1, to(-2)),
        along(own.at[:, 1:2], g.at[0:3, top + 1 : top + 2, rows], 2, 2, to(-2)),
    )
    via = (
        along(chem_h.at[:, 0:2], relay.at[3:5], 0, 13, to(2)),
        along(own.at[:, 0:1], relay.at[0:3, 0:1], 1, 14, to(2)),
        along(own.at[:, 1:2], relay.at[0:3, 1:2], 2, 15, to(2)),
    )
    far = (
        along(relay.at[3:5], g.at[3:5, top : top + 2, rows], 13, 0, to(-4)),
        along(relay.at[0:3, 0:1], g.at[0:3, top : top + 1, rows], 14, 1, to(-4)),
        along(relay.at[0:3, 1:2], g.at[0:3, top + 1 : top + 2, rows], 15, 2, to(-4)),
    )
    head_chem = along(chem_h.at[:, 0:2], g.at[3:5, 2:4, rows], 3, 3, to(-1))
    lead_chem = along(chem_h.at[:, 2:4], g.at[3:5, 4:6, rows], 16, 16, to(-1))
    body_chem = along(chem_h.at[:, 4:cz], g.at[3:5, 6:top, rows], 4, 4, to(-1))
    def banded(src, dst, send, recv, device):
        return [
            along(src(planes, band), dst(planes, band), send + k, recv + k, device)
            for k, (planes, band) in enumerate(
                ((pl.ds(0, 2), low), (pl.ds(0, 2), high), (pl.ds(0, 1), middle), (pl.ds(1, 1), middle)))
        ]

    final_own, final_g = own.at[:, cz - 2 : cz], g.at[0:3, cz:top]
    last_phi = banded(lambda p, r: final_own.at[:, p, r], lambda p, r: final_g.at[:, p, r], 5, 5, to(-1))
    end_g, head_g = g.at[0:3, top : top + 2], g.at[0:3, 2:4]
    pass_chem = along(g.at[3:5, top : top + 2, rows], g.at[3:5, 2:4, rows], 17, 3, to(1))
    pass_phi = banded(lambda p, r: end_g.at[:, p, r], lambda p, r: head_g.at[:, p, r], 9, 9, to(1))
    pass_phi = [pass_phi[0], pass_phi[1], pass_phi[3], pass_phi[2]]

    def plane_phi(p):
        return pltpu.make_async_remote_copy(
            src_ref=own.at[:, pl.ds(p, 1)], dst_ref=g.at[0:3, pl.ds(p + 2, 1), rows],
            send_sem=plane_send.at[p], recv_sem=plane_recv.at[p],
            device_id={"grow": to(-1)}, device_id_type=MESH)

    gives_end = jnp.logical_and(me > 1, corner != 0)
    even_end = jnp.logical_and(corner == 2, me > 1)
    odd_end = jnp.logical_and(odd, me > 1)

    @pl.when(odd)
    def _():
        head_chem.start()

    @pl.when(gives)
    def _():
        lead_chem.start()
        body_chem.start()

    @pl.when(even_end)
    def _():
        end[0].start()

    @pl.when(gives_via)
    def _():
        via[0].start()

    loads[0].wait()
    loads[1].wait()

    def initial(p, _):
        kind = labels[p]
        weights = [blend[a, p] for a in range(4)]
        inverse = 1.0 / (1.0 + ((weights[0] + weights[1]) + (weights[2] + weights[3])))
        for a in range(3):
            own[a, p] = (jnp.where(kind == a, 1.0, 0.0) + weights[a]) * inverse
        return _

    lax.fori_loop(0, cz, initial, None)

    @pl.when(odd)
    def _():
        plane_phi(0).start()
        plane_phi(1).start()

    @pl.when(even_end)
    def _():
        end[1].start()
        end[2].start()

    @pl.when(gives_via)
    def _():
        via[1].start()
        via[2].start()

    def planes(low_p, high_p, act):
        def step(p, _):
            act(plane_phi(p))
            return _

        lax.fori_loop(low_p, high_p, step, None)

    @pl.when(gives)
    def _():
        planes(2, cz - 2, lambda copy: copy.start())
        for copy in last_phi:
            copy.start()

    for k in range(2):
        for a in range(3):
            g[a, k, 0:nx] = own[a, cz - 2 + k]

    @pl.when(odd)
    def _():
        pl.semaphore_wait(go, 1)

    loads[2].wait()
    loads[3].wait()
    loads[4].wait()

    @pl.when(gets_via)
    def _():
        for landed, onward in zip(via, far):
            landed.wait_recv()
            onward.start()

    def sideways(fields, planes, group):
        return (
            pltpu.make_async_remote_copy(
                src_ref=g.at[fields, planes, nx - ROWS : nx], dst_ref=from_left.at[fields, planes],
                send_sem=lat_send.at[0, group], recv_sem=lat_recv.at[0, group],
                device_id={"lat": right}, device_id_type=MESH),
            pltpu.make_async_remote_copy(
                src_ref=g.at[fields, planes, 0:ROWS], dst_ref=from_right.at[fields, planes],
                send_sem=lat_send.at[1, group], recv_sem=lat_recv.at[1, group],
                device_id={"lat": left}, device_id_type=MESH),
        )

    everything, phases, chemical = slice(0, 5), slice(0, 3), slice(3, 5)
    lat_own = sideways(everything, slice(1, 2), 0)
    lat_head_chem = sideways(chemical, slice(2, 4), 1)
    lat_end_chem = sideways(chemical, slice(top, top + 1), 2)
    lat_chem = sideways(chemical, slice(4, top), 3)

    lat_pair = sideways(phases, slice(cz, top), 4 + cz - 2)
    lat_head = sideways(phases, slice(2, 4), 4 + cz - 1)

    def lat_plane(p):
        return sideways(phases, pl.ds(p + 2, 1), 4 + p)

    def start(pair):
        for copy in pair:
            copy.start()

    def wait(pair):
        for copy in pair:
            copy.wait()

    def merge(fields, z):
        for f in fields:
            g[f, z, nx : nx + ROWS] = jnp.where(row < 4, from_right[f, z], from_left[f, z])

    def first(z, parts):
        for t in parts:
            new, chem = tile_step(g, z, t, tiles, (me + 1) * cz - 2 + z, n * cz)
            for f, value in enumerate(new[:3] + chem):
                half[f, z, t * ROWS : (t + 1) * ROWS] = value

    def second(z):
        for t in inner:
            new, chem = tile_step(half, z, t, tiles, (me + 1) * cz - 2 + z, n * cz)
            for f, value in enumerate(new + chem):
                staged[f, z - 2, t * ROWS : (t + 1) * ROWS] = value

    def chem_in():
        start(lat_own)
        body_chem.wait_recv()
        start(lat_chem)
        wait(lat_own)
        merge(range(5), 1)
        wait(lat_chem)
        lax.fori_loop(4, top, lambda z, _: merge((3, 4), z), None)

    def head_chem_lands():
        wait(lat_head_chem)
        lax.fori_loop(2, 4, lambda z, _: merge((3, 4), z), None)

    @pl.when(jnp.logical_and(even, gets_end))
    def _():
        end[0].wait_recv()
        pass_chem.start()
        start(lat_end_chem)
        end[1].wait_recv()
        start(lat_plane(cz))
        end[2].wait_recv()
        for copy in pass_phi:
            copy.start()

    @pl.when(gets)
    def _():
        lead_chem.wait_recv()

    @pl.when(odd_end)
    def _():
        for copy in end:
            copy.start()

    @pl.when(gets)
    def _():
        chem_in()

    @pl.when(jnp.logical_and(gets, even))
    def _():
        head_chem.wait_recv()
        start(lat_head_chem)
        head_chem_lands()

    code = jnp.where(even, 0, jnp.where(corner == 1, 1, 2))
    plans = [schedule(kind, cz) for kind in range(3)]
    words = []
    for k in range(max(len(plan) for plan in plans)):
        packed = [pack(plan[k]) if k < len(plan) else (0, 0) for plan in plans]
        words.append([jnp.where(code == 0, p0, jnp.where(code == 1, p1, p2)) for p0, p1, p2 in zip(*packed)])
    count = jnp.where(code == 0, len(plans[0]), jnp.where(code == 1, len(plans[1]), len(plans[2])))
    count = jnp.where(gets, count, 0)
    topmost = jnp.logical_not(gets_end)

    def run(k, _):
        comm, work = pick(k, [w[0] for w in words]), pick(k, [w[1] for w in words])
        event, sent, landed = comm % BASE, comm // BASE % BASE, comm // (BASE * BASE)

        def span(value):
            low_z = value % BASE
            return low_z, low_z + value // BASE

        h0, h1 = span(work % (4 * BASE))
        f0, f1 = span(work // (4 * BASE) % (4 * BASE))
        s0, s1 = span(work // (16 * BASE * BASE))

        @pl.when(event == PLANE)
        def _():
            plane_phi(sent - 1).wait_recv()

        @pl.when(event == EDGES)
        def _():
            last_phi[0].wait_recv()
            last_phi[1].wait_recv()
            start(lat_pair)

        @pl.when(event == MID)
        def _():
            last_phi[2].wait_recv()

        @pl.when(event == LAST)
        def _():
            last_phi[3].wait_recv()

        @pl.when(event == HEAD)
        def _():
            head_chem.wait_recv()
            start(lat_head_chem)
            pass_phi[0].wait_recv()
            pass_phi[1].wait_recv()
            start(lat_head)

        @pl.when(event == PASS_MID)
        def _():
            pass_phi[2].wait_recv()

        @pl.when(event == PASS_LAST)
        def _():
            pass_phi[3].wait_recv()

        @pl.when(event == END)
        def _():
            end[0].wait_recv()
            start(lat_end_chem)
            end[1].wait_recv()

        @pl.when(event == END_NEXT)
        def _():
            end[2].wait_recv()

        @pl.when(jnp.logical_or(event == PLANE, event == END))
        def _():
            start(lat_plane(sent - 1))

        ending = landed == cz + 1

        @pl.when(jnp.logical_and(ending, gets_end))
        def _():
            wait(lat_end_chem)
            merge((3, 4), top)

        @pl.when(jnp.logical_or(jnp.logical_and(landed > 0, landed < cz - 1), jnp.logical_and(ending, gets_end)))
        def _():
            wait(lat_plane(landed - 1))
            merge(range(3), landed + 1)

        @pl.when(landed == cz - 1)
        def _():
            wait(lat_pair)
            lax.fori_loop(cz, top, lambda z, _: merge(range(3), z), None)

        @pl.when(landed == cz)
        def _():
            head_chem_lands()
            wait(lat_head)
            lax.fori_loop(2, 4, lambda z, _: merge(range(3), z), None)

        @pl.when(jnp.logical_and(topmost, landed == cz - 1))
        def _():
            for f in range(5):
                g[f, top, nx:] = g[f, top - 1, nx:]

        @pl.when(jnp.logical_and(topmost, event == LAST))
        def _():
            for f in range(5):
                g[f, top, 0:nx] = g[f, top - 1, 0:nx]

        lax.fori_loop(h0, h1, lambda z, _: first(z, (tiles,)), None)
        lax.fori_loop(f0, jnp.minimum(f1, jnp.where(topmost, top, top + 1)), lambda z, _: first(z, inner), None)

        @pl.when(jnp.logical_and(topmost, event == LAST))
        def _():
            for f in range(5):
                half[f, top, 0:nx] = half[f, top - 1, 0:nx]

        lax.fori_loop(s0, jnp.minimum(s1, cz + 2 - LATE), lambda z, _: second(z), None)
        return _

    lax.fori_loop(0, count, run, None)

    @pl.when(jnp.logical_not(gets))
    def _():
        def entering(o, _):
            kind = index[o]
            for a in range(4):
                staged[a, o] = jnp.full((nx, ny), 1.0 if a == 0 else 0.0, jnp.float32)
            for k in range(2):
                value = jnp.zeros((nx, ny), jnp.float32)
                for liquid in range(table.shape[1]):
                    value = jnp.where(kind == liquid, table[k, liquid], value)
                staged[4 + k, o] = value
            return _

        lax.fori_loop(0, cz, entering, None)

    @pl.when(gives_end)
    def _():
        for copy in end:
            copy.wait_send()

    @pl.when(gives_via)
    def _():
        for copy in via:
            copy.wait_send()

    @pl.when(gets_via)
    def _():
        for copy in far:
            copy.wait_send()

    @pl.when(odd)
    def _():
        head_chem.wait_send()
        plane_phi(0).wait_send()
        plane_phi(1).wait_send()

    @pl.when(gives)
    def _():
        lead_chem.wait_send()
        body_chem.wait_send()
        planes(2, cz - 2, lambda copy: copy.wait_send())
        for copy in last_phi:
            copy.wait_send()

    @pl.when(jnp.logical_and(even, gets_end))
    def _():
        pass_chem.wait_send()
        for copy in pass_phi:
            copy.wait_send()


def flush(n, staged, half, phase_out, chem_out, final, sem):
    cz, nx = staged.shape[1:3]
    early, tiles = cz - LATE, nx // ROWS
    me = lax.axis_index("grow")

    def out(src, low, count, k):
        return (
            pltpu.make_async_copy(src.at[0:4], phase_out.at[:, pl.ds(low, count)], sem.at[0, k]),
            pltpu.make_async_copy(src.at[4:6], chem_out.at[:, pl.ds(low, count)], sem.at[1, k]),
        )

    first_part = out(staged.at[:, 0:early], 0, early, LATE)
    for copy in first_part:
        copy.start()

    def late(q):
        return out(final.at[:, pl.ds(q, 1)], early + q, 1, q)

    def plane(q, _):
        z = q + early + 2

        @pl.when(me < n - 1)
        def _():
            for t in range(tiles):
                new, chem = tile_step(half, z, t, tiles, (me + 1) * cz - 2 + z, n * cz)
                for f, value in enumerate(new + chem):
                    final[f, q, t * ROWS : (t + 1) * ROWS] = value

        @pl.when(me == n - 1)
        def _():
            for f in range(6):
                final[f, q] = staged[f, early + q]

        for copy in late(q):
            copy.start()
        return _

    lax.fori_loop(0, LATE, plane, None)
    for copy in first_part:
        copy.wait()

    def written(q, _):
        for copy in late(q):
            copy.wait()
        return _

    lax.fori_loop(0, LATE, written, None)


def body(labels, seed_blend, potential, inflow_index, liquid_table):
    n, m = lax.axis_size("grow"), lax.axis_size("lat")
    cz, nx, ny = labels.shape
    dma = pltpu.SemaphoreType.DMA
    f32 = jnp.float32
    vmem, hbm = pl.BlockSpec(memory_space=pltpu.VMEM), pl.BlockSpec(memory_space=pltpu.HBM)
    state = pl.pallas_call(
        functools.partial(kernel, n, m),
        out_shape=(pltpu.VMEM((6, cz, nx, ny), f32), pltpu.VMEM((5, cz + 4, nx + ROWS, ny), f32)),
        in_specs=[hbm] * 5,
        out_specs=(vmem, vmem),
        scratch_shapes=[
            pltpu.SMEM(liquid_table.shape[::-1], f32),
            pltpu.VMEM((cz, nx, ny), jnp.int32),
            pltpu.VMEM((4, cz, nx, ny), f32),
            pltpu.VMEM((cz, nx, ny), jnp.int32),
            pltpu.VMEM((3, cz, nx, ny), f32),
            pltpu.VMEM((5, cz + 4, nx + ROWS, ny), f32),
            pltpu.VMEM((5, cz + 4, ROWS, ny), f32),
            pltpu.VMEM((5, cz + 4, ROWS, ny), f32),
            pltpu.VMEM((5, 2, nx, ny), f32),
            dma((5,)),
            dma((18,)),
            dma((17,)),
            dma((cz,)),
            dma((cz,)),
            dma((2, 5 + cz)),
            dma((2, 5 + cz)),
            pltpu.SemaphoreType.REGULAR,
        ],
        compiler_params=pltpu.CompilerParams(collective_id=0, has_side_effects=True, vmem_limit_bytes=12 << 20),
    )(*(pltpu.with_memory_space_constraint(a, pltpu.HBM) for a in (labels, seed_blend, potential, inflow_index, liquid_table.T)))
    return pl.pallas_call(
        functools.partial(flush, n),
        out_shape=(jax.ShapeDtypeStruct((4, cz, nx, ny), f32), jax.ShapeDtypeStruct((2, cz, nx, ny), f32)),
        in_specs=[vmem, vmem],
        out_specs=(hbm, hbm),
        scratch_shapes=[pltpu.VMEM((6, LATE, nx, ny), f32), dma((2, LATE + 1))],
        compiler_params=pltpu.CompilerParams(vmem_limit_bytes=4 << 20),
    )(*(pltpu.with_memory_space_constraint(a, pltpu.VMEM) for a in state))


def solution(mesh):
    in_specs = (
        P("grow", "lat", None),
        P(None, "grow", "lat", None),
        P(None, "grow", "lat", None),
        P(None, "lat", None),
        P(),
    )
    out_specs = (P(None, "grow", "lat", None), P(None, "grow", "lat", None))
    return jax.shard_map(body, mesh=mesh, in_specs=in_specs, out_specs=out_specs, check_vma=False)
```

```python
import functools

import jax
import jax.numpy as jnp
from jax import lax
from jax.experimental import pallas as pl
from jax.experimental.pallas import tpu as pltpu
from jax.sharding import PartitionSpec as P

offset_table = ((0.0, 0.0), (0.6, -0.3), (-0.4, 0.5), (-0.2, -0.6))
latent_heat = (0.0, 0.8, 0.8, 0.8)
relax_rate = 0.1
diffusion = 0.05
MESH = pl.DeviceIdType.MESH
ROWS = 8
LATE = 3


def advance(phi, chem, lap, temp):
    phi = list(phi) + [1.0 - (phi[0] + phi[1] + phi[2])]
    square = chem[0] * chem[0] + chem[1] * chem[1]
    pull = []
    for a in range(4):
        e0, e1 = offset_table[a]
        p = phi[a]
        w = square - (1.0 - p) * (1.0 - 2.0 * p)
        if a:
            w = w + ((2.0 * e0) * chem[0] + (2.0 * e1) * chem[1] + ((e0 * e0 + e1 * e1) - 2.0 * latent_heat[a] * temp))
        pull.append(p * w)
    mean = 0.25 * ((pull[0] + pull[1]) + (pull[2] + pull[3]))
    new = [phi[a] + relax_rate * ((lap[a] + pull[a]) - mean) for a in range(3)]
    new.append(1.0 - (new[0] + new[1] + new[2]))
    squares = [v * v for v in new]
    growth = [squares[a] - phi[a] * phi[a] for a in range(4)]
    total = (growth[0] + growth[1]) + (growth[2] + growth[3])
    inverse = 1.0 / ((squares[0] + squares[1]) + (squares[2] + squares[3]))
    mobile = diffusion * (0.1 + squares[0])
    out = []
    for k in range(2):
        source = chem[k] * total
        for a in range(1, 4):
            source = source + offset_table[a][k] * growth[a]
        out.append(chem[k] + (mobile * lap[3 + k] - source) * inverse)
    return new, out


def tile_step(src, z, t, tiles, plane, planes):
    ny = src.shape[-1]
    row = lax.broadcasted_iota(jnp.int32, (ROWS, ny), 0)

    def part(f, z, t):
        return src[f, z, t * ROWS : (t + 1) * ROWS]

    after, before = (t + 1) % (tiles + 1), (t + tiles) % (tiles + 1)
    centre, lap = [], []
    for f in range(5):
        c = part(f, z, t)
        up = pltpu.roll(jnp.where(row == 0, part(f, z, after), c), ROWS - 1, 0)
        down = pltpu.roll(jnp.where(row == ROWS - 1, part(f, z, before), c), 1, 0)
        lap.append(
            ((part(f, z + 1, t) + part(f, z - 1, t)) + (up + down))
            + (pltpu.roll(c, ny - 1, 1) + pltpu.roll(c, 1, 1)) - 6.0 * c)
        centre.append(c)
    temp = 2.0 * (plane.astype(jnp.float32) + 0.5) / float(planes) - 1.0
    return advance(centre[:3], centre[3:], lap, temp)


PLANE, EDGES, MID, LAST, HEAD, PASS_MID, PASS_LAST, END, END_NEXT, BOTH = range(1, 11)


def schedule(kind, cz):
    pair, head, top = cz - 2, cz - 1, cz + 2
    none = (0, 0)

    def step(event, sent=None, landed=None, halo=none, own=none, two=none):
        return (event, 0 if sent is None else sent + 1, 0 if landed is None else landed + 1, halo, own, two)

    if kind == 0:
        return [
            step(PLANE, 0, cz),
            step(PLANE, 1, 0, none, (1, 1)),
            step(PLANE, 2, 1, (2, 1), (2, 1)),
            *(step(PLANE, p, p - 1, (p, 1), (p, 1), (p - 1, 1)) for p in range(3, pair)),
            step(EDGES, pair, pair - 1, (pair, 1), (pair, 1), (pair - 1, 1)),
            step(0, None, pair, (pair + 1, 3)),
            step(MID, None, None, none, (pair + 1, 1), (pair, 1)),
            step(LAST, None, None, none, (cz, 3), (cz - 1, 3)),
        ]
    body = [step(PLANE, 2), step(PLANE, 3, 2)]
    if kind == 1:
        return [
            *body,
            step(PLANE, 4, 3),
            step(PLANE, 5, 4, (5, 1), (5, 1)),
            *(step(PLANE, p, p - 1, (p, 1), (p, 1), (p - 1, 1) if p > 6 else none) for p in range(6, pair)),
            step(EDGES, pair, pair - 1, (pair, 1), (pair, 1), (pair - 1, 1) if pair > 6 else none),
            step(0, None, pair, (pair + 1, 2)),
            step(MID, None, None, none, (pair + 1, 1), (pair, 1)),
            step(LAST, None, None, none, (cz, 1), (cz - 1, 1)),
            step(HEAD, head),
            step(0, None, head, (2, 3)),
            step(PASS_MID, None, None, none, (4, 1), (5, 1)),
            step(PASS_LAST, None, None, none, (1, 3), (2, 3)),
            step(END, cz),
            step(0, None, cz, (cz + 1, 1), (cz + 1, 1), (cz, 1)),
            step(END_NEXT, None, None, none, (top, 1), (cz + 1, 1)),
        ]
    return [
        *body,
        step(END, cz, 3),
        step(PLANE, 4, cz),
        step(END_NEXT, None, 4, (5, 1), (5, 1)),
        step(PLANE, 5),
        *(step(PLANE, p, p - 1, (p, 1), (p, 1), (p - 1, 1) if p > 6 else none) for p in range(6, pair)),
        step(HEAD, head, pair - 1, (pair, 1), (pair, 1), (pair - 1, 1) if pair > 6 else none),
        step(PASS_MID, None, head, (2, 3), (4, 1), (5, 1)),
        step(EDGES, pair),
        step(PASS_LAST, None, None, none, (1, 3), (2, 3)),
        step(BOTH, None, pair, (pair + 1, 3), (pair + 1, 4), (pair, 4)),
    ]


BASE = 32


def pack(step):
    event, sent, landed, halo, own, two = step
    work = 0
    for low, number in (two, own, halo):
        work = work * (8 * BASE) + low + BASE * number
    return event + BASE * (sent + BASE * landed), work


def pick(k, values):
    bit = 1
    while len(values) > 1:
        odd = k // bit % 2 == 1
        paired = [jnp.where(odd, b, a) for a, b in zip(values[0::2], values[1::2])]
        values = paired + values[len(values) - len(values) % 2 :]
        bit *= 2
    return values[0]


def kernel(n, m, labels_h, blend_h, chem_h, index_h, table_h, staged, half,
           table, labels, blend, index, own, g, from_right, from_left, relay,
           load_sem, send_sem, recv_sem, plane_send, plane_recv, lat_send, lat_recv, go):
    cz, nx, ny = labels.shape
    tiles = nx // ROWS
    inner = tuple(range(tiles))
    top = cz + 2
    me = lax.axis_index("grow")
    lat = lax.axis_index("lat")
    right, left = lax.rem(lat + 1, m), lax.rem(lat + m - 1, m)
    corner = lax.rem(me, 4)
    even = lax.rem(me, 2) == 0
    odd = jnp.logical_not(even)
    gives, gets = me > 0, me < n - 1
    gets_end = me < n - 2
    gives_via = jnp.logical_and(corner == 0, me > 0)
    gets_via = jnp.logical_and(corner == 2, me > 4)
    row = lax.broadcasted_iota(jnp.int32, (ROWS, ny), 0)

    barrier = pltpu.get_barrier_semaphore()

    def greet(there, device):
        @pl.when(there)
        def _():
            pl.semaphore_signal(barrier, inc=1, device_id={"grow": device}, device_id_type=MESH)

    greet(odd, me - 1)
    greet(even, me + 1)
    greet(jnp.logical_and(odd, me + 1 < n), me + 1)
    greet(corner == 0, me + 2)
    greet(gets_via, me - 2)
    greet(jnp.logical_and(corner == 2, me + 4 < n), me + 4)
    for side in (left, right):
        pl.semaphore_signal(barrier, inc=1, device_id={"lat": side}, device_id_type=MESH)

    loads = [
        pltpu.make_async_copy(labels_h, labels, load_sem.at[0]),
        pltpu.make_async_copy(blend_h, blend, load_sem.at[1]),
        pltpu.make_async_copy(index_h, index, load_sem.at[2]),
        pltpu.make_async_copy(chem_h.at[:, cz - 2 : cz], g.at[3:5, 0:2, 0:nx], load_sem.at[3]),
        pltpu.make_async_copy(table_h, table, load_sem.at[4]),
    ]
    for load in loads:
        load.start()

    met = 3 + jnp.where(even, (me > 0).astype(jnp.int32) + (corner == 2).astype(jnp.int32)
                        + gets_via.astype(jnp.int32) + gives_via.astype(jnp.int32), 0)
    pl.semaphore_wait(barrier, met)

    @pl.when(even)
    def _():
        pl.semaphore_signal(go, inc=1, device_id={"grow": me + 1}, device_id_type=MESH)

    def to(step):
        return lax.rem(me + n + step, n)

    def along(src, dst, send, recv, device):
        return pltpu.make_async_remote_copy(
            src_ref=src, dst_ref=dst, send_sem=send_sem.at[send], recv_sem=recv_sem.at[recv],
            device_id={"grow": device}, device_id_type=MESH)

    low, middle, high = pl.ds(0, ROWS), pl.ds(ROWS, nx - 2 * ROWS), pl.ds(nx - ROWS, ROWS)
    rows = pl.ds(0, nx)

    end = (
        along(chem_h.at[:, 0:2], g.at[3:5, top : top + 2, rows], 0, 0, to(-2)),
        along(own.at[:, 0:1], g.at[0:3, top : top + 1, rows], 1, 1, to(-2)),
        along(own.at[:, 1:2], g.at[0:3, top + 1 : top + 2, rows], 2, 2, to(-2)),
    )
    via = (
        along(chem_h.at[:, 0:2], relay.at[3:5], 0, 13, to(2)),
        along(own.at[:, 0:1], relay.at[0:3, 0:1], 1, 14, to(2)),
        along(own.at[:, 1:2], relay.at[0:3, 1:2], 2, 15, to(2)),
    )
    far = (
        along(relay.at[3:5], g.at[3:5, top : top + 2, rows], 13, 0, to(-4)),
        along(relay.at[0:3, 0:1], g.at[0:3, top : top + 1, rows], 14, 1, to(-4)),
        along(relay.at[0:3, 1:2], g.at[0:3, top + 1 : top + 2, rows], 15, 2, to(-4)),
    )
    head_chem = along(chem_h.at[:, 0:2], g.at[3:5, 2:4, rows], 3, 3, to(-1))
    lead_chem = along(chem_h.at[:, 2:4], g.at[3:5, 4:6, rows], 16, 16, to(-1))
    body_chem = along(chem_h.at[:, 4:cz], g.at[3:5, 6:top, rows], 4, 4, to(-1))
    def banded(src, dst, send, recv, device):
        return [
            along(src(planes, band), dst(planes, band), send + k, recv + k, device)
            for k, (planes, band) in enumerate(
                ((pl.ds(0, 2), low), (pl.ds(0, 2), high), (pl.ds(0, 1), middle), (pl.ds(1, 1), middle)))
        ]

    final_own, final_g = own.at[:, cz - 2 : cz], g.at[0:3, cz:top]
    last_phi = banded(lambda p, r: final_own.at[:, p, r], lambda p, r: final_g.at[:, p, r], 5, 5, to(-1))
    end_g, head_g = g.at[0:3, top : top + 2], g.at[0:3, 2:4]
    pass_chem = along(g.at[3:5, top : top + 2, rows], g.at[3:5, 2:4, rows], 17, 3, to(1))
    pass_phi = banded(lambda p, r: end_g.at[:, p, r], lambda p, r: head_g.at[:, p, r], 9, 9, to(1))
    pass_phi = [pass_phi[0], pass_phi[1], pass_phi[3], pass_phi[2]]

    def plane_phi(p):
        return pltpu.make_async_remote_copy(
            src_ref=own.at[:, pl.ds(p, 1)], dst_ref=g.at[0:3, pl.ds(p + 2, 1), rows],
            send_sem=plane_send.at[p], recv_sem=plane_recv.at[p],
            device_id={"grow": to(-1)}, device_id_type=MESH)

    gives_end = jnp.logical_and(me > 1, corner != 0)
    even_end = jnp.logical_and(corner == 2, me > 1)
    odd_end = jnp.logical_and(odd, me > 1)

    @pl.when(odd)
    def _():
        head_chem.start()

    @pl.when(gives)
    def _():
        lead_chem.start()
        body_chem.start()

    @pl.when(even_end)
    def _():
        end[0].start()

    @pl.when(gives_via)
    def _():
        via[0].start()

    loads[0].wait()
    loads[1].wait()

    def initial(p, _):
        kind = labels[p]
        weights = [blend[a, p] for a in range(4)]
        inverse = 1.0 / (1.0 + ((weights[0] + weights[1]) + (weights[2] + weights[3])))
        for a in range(3):
            own[a, p] = (jnp.where(kind == a, 1.0, 0.0) + weights[a]) * inverse
        return _

    lax.fori_loop(0, cz, initial, None)

    @pl.when(odd)
    def _():
        plane_phi(0).start()
        plane_phi(1).start()

    @pl.when(even_end)
    def _():
        end[1].start()
        end[2].start()

    @pl.when(gives_via)
    def _():
        via[1].start()
        via[2].start()

    def planes(low_p, high_p, act):
        def step(p, _):
            act(plane_phi(p))
            return _

        lax.fori_loop(low_p, high_p, step, None)

    @pl.when(gives)
    def _():
        planes(2, cz - 2, lambda copy: copy.start())
        for copy in last_phi:
            copy.start()

    for k in range(2):
        for a in range(3):
            g[a, k, 0:nx] = own[a, cz - 2 + k]

    @pl.when(odd)
    def _():
        pl.semaphore_wait(go, 1)

    loads[2].wait()
    loads[3].wait()
    loads[4].wait()

    @pl.when(gets_via)
    def _():
        for landed, onward in zip(via, far):
            landed.wait_recv()
            onward.start()

    def sideways(fields, planes, group):
        return (
            pltpu.make_async_remote_copy(
                src_ref=g.at[fields, planes, nx - ROWS : nx], dst_ref=from_left.at[fields, planes],
                send_sem=lat_send.at[0, group], recv_sem=lat_recv.at[0, group],
                device_id={"lat": right}, device_id_type=MESH),
            pltpu.make_async_remote_copy(
                src_ref=g.at[fields, planes, 0:ROWS], dst_ref=from_right.at[fields, planes],
                send_sem=lat_send.at[1, group], recv_sem=lat_recv.at[1, group],
                device_id={"lat": left}, device_id_type=MESH),
        )

    everything, phases, chemical = slice(0, 5), slice(0, 3), slice(3, 5)
    lat_own = sideways(everything, slice(1, 2), 0)
    lat_head_chem = sideways(chemical, slice(2, 4), 1)
    lat_end_chem = sideways(chemical, slice(top, top + 1), 2)
    lat_chem = sideways(chemical, slice(4, top), 3)

    lat_pair = sideways(phases, slice(cz, top), 4 + cz - 2)
    lat_head = sideways(phases, slice(2, 4), 4 + cz - 1)

    def lat_plane(p):
        return sideways(phases, pl.ds(p + 2, 1), 4 + p)

    def start(pair):
        for copy in pair:
            copy.start()

    def wait(pair):
        for copy in pair:
            copy.wait()

    def merge(fields, z):
        for f in fields:
            g[f, z, nx : nx + ROWS] = jnp.where(row < 4, from_right[f, z], from_left[f, z])

    def first(z, parts):
        for t in parts:
            new, chem = tile_step(g, z, t, tiles, (me + 1) * cz - 2 + z, n * cz)
            for f, value in enumerate(new[:3] + chem):
                half[f, z, t * ROWS : (t + 1) * ROWS] = value

    def second(z):
        for t in inner:
            new, chem = tile_step(half, z, t, tiles, (me + 1) * cz - 2 + z, n * cz)
            for f, value in enumerate(new + chem):
                staged[f, z - 2, t * ROWS : (t + 1) * ROWS] = value

    def chem_in():
        start(lat_own)
        body_chem.wait_recv()
        start(lat_chem)
        wait(lat_own)
        merge(range(5), 1)
        wait(lat_chem)
        lax.fori_loop(4, top, lambda z, _: merge((3, 4), z), None)

    def head_chem_lands():
        wait(lat_head_chem)
        lax.fori_loop(2, 4, lambda z, _: merge((3, 4), z), None)

    @pl.when(jnp.logical_and(even, gets_end))
    def _():
        end[0].wait_recv()
        pass_chem.start()
        start(lat_end_chem)
        end[1].wait_recv()
        start(lat_plane(cz))
        end[2].wait_recv()
        for copy in pass_phi:
            copy.start()

    @pl.when(gets)
    def _():
        lead_chem.wait_recv()

    @pl.when(odd_end)
    def _():
        for copy in end:
            copy.start()

    @pl.when(gets)
    def _():
        chem_in()

    @pl.when(jnp.logical_and(gets, even))
    def _():
        head_chem.wait_recv()
        start(lat_head_chem)
        head_chem_lands()

    code = jnp.where(even, 0, jnp.where(corner == 1, 1, 2))
    plans = [schedule(kind, cz) for kind in range(3)]
    words = []
    for k in range(max(len(plan) for plan in plans)):
        packed = [pack(plan[k]) if k < len(plan) else (0, 0) for plan in plans]
        words.append([jnp.where(code == 0, p0, jnp.where(code == 1, p1, p2)) for p0, p1, p2 in zip(*packed)])
    count = jnp.where(code == 0, len(plans[0]), jnp.where(code == 1, len(plans[1]), len(plans[2])))
    count = jnp.where(gets, count, 0)
    topmost = jnp.logical_not(gets_end)

    def run(k, _):
        comm, work = pick(k, [w[0] for w in words]), pick(k, [w[1] for w in words])
        event, sent, landed = comm % BASE, comm // BASE % BASE, comm // (BASE * BASE)

        def span(value):
            low_z = value % BASE
            return low_z, low_z + value // BASE

        h0, h1 = span(work % (8 * BASE))
        f0, f1 = span(work // (8 * BASE) % (8 * BASE))
        s0, s1 = span(work // (64 * BASE * BASE))

        @pl.when(event == PLANE)
        def _():
            plane_phi(sent - 1).wait_recv()

        @pl.when(event == EDGES)
        def _():
            last_phi[0].wait_recv()
            last_phi[1].wait_recv()
            start(lat_pair)

        @pl.when(jnp.logical_or(event == MID, event == BOTH))
        def _():
            last_phi[2].wait_recv()

        @pl.when(jnp.logical_or(event == LAST, event == BOTH))
        def _():
            last_phi[3].wait_recv()

        @pl.when(event == HEAD)
        def _():
            head_chem.wait_recv()
            start(lat_head_chem)
            pass_phi[0].wait_recv()
            pass_phi[1].wait_recv()
            start(lat_head)

        @pl.when(event == PASS_MID)
        def _():
            pass_phi[2].wait_recv()

        @pl.when(event == PASS_LAST)
        def _():
            pass_phi[3].wait_recv()

        @pl.when(event == END)
        def _():
            end[0].wait_recv()
            start(lat_end_chem)
            end[1].wait_recv()

        @pl.when(event == END_NEXT)
        def _():
            end[2].wait_recv()

        @pl.when(jnp.logical_or(event == PLANE, event == END))
        def _():
            start(lat_plane(sent - 1))

        ending = landed == cz + 1

        @pl.when(jnp.logical_and(ending, gets_end))
        def _():
            wait(lat_end_chem)
            merge((3, 4), top)

        @pl.when(jnp.logical_or(jnp.logical_and(landed > 0, landed < cz - 1), jnp.logical_and(ending, gets_end)))
        def _():
            wait(lat_plane(landed - 1))
            merge(range(3), landed + 1)

        @pl.when(landed == cz - 1)
        def _():
            wait(lat_pair)
            lax.fori_loop(cz, top, lambda z, _: merge(range(3), z), None)

        @pl.when(landed == cz)
        def _():
            head_chem_lands()
            wait(lat_head)
            lax.fori_loop(2, 4, lambda z, _: merge(range(3), z), None)

        @pl.when(jnp.logical_and(topmost, landed == cz - 1))
        def _():
            for f in range(5):
                g[f, top, nx:] = g[f, top - 1, nx:]

        @pl.when(jnp.logical_and(topmost, event == LAST))
        def _():
            for f in range(5):
                g[f, top, 0:nx] = g[f, top - 1, 0:nx]

        def halo_pair(q, _):
            for step in range(2):
                first(h0 + 2 * q + step, (tiles,))
            return _

        lax.fori_loop(0, (h1 - h0) // 2, halo_pair, None)
        lax.fori_loop(h1 - (h1 - h0) % 2, h1, lambda z, _: first(z, (tiles,)), None)
        lax.fori_loop(f0, jnp.minimum(f1, jnp.where(topmost, top, top + 1)), lambda z, _: first(z, inner), None)

        @pl.when(jnp.logical_and(topmost, event == LAST))
        def _():
            for f in range(5):
                half[f, top, 0:nx] = half[f, top - 1, 0:nx]

        lax.fori_loop(s0, jnp.minimum(s1, cz + 2 - LATE), lambda z, _: second(z), None)
        return _

    lax.fori_loop(0, count, run, None)

    @pl.when(jnp.logical_not(gets))
    def _():
        def entering(o, _):
            kind = index[o]
            for a in range(4):
                staged[a, o] = jnp.full((nx, ny), 1.0 if a == 0 else 0.0, jnp.float32)
            for k in range(2):
                value = jnp.zeros((nx, ny), jnp.float32)
                for liquid in range(table.shape[1]):
                    value = jnp.where(kind == liquid, table[k, liquid], value)
                staged[4 + k, o] = value
            return _

        lax.fori_loop(0, cz, entering, None)

    @pl.when(gives_end)
    def _():
        for copy in end:
            copy.wait_send()

    @pl.when(gives_via)
    def _():
        for copy in via:
            copy.wait_send()

    @pl.when(gets_via)
    def _():
        for copy in far:
            copy.wait_send()

    @pl.when(odd)
    def _():
        head_chem.wait_send()
        plane_phi(0).wait_send()
        plane_phi(1).wait_send()

    @pl.when(gives)
    def _():
        lead_chem.wait_send()
        body_chem.wait_send()
        planes(2, cz - 2, lambda copy: copy.wait_send())
        for copy in last_phi:
            copy.wait_send()

    @pl.when(jnp.logical_and(even, gets_end))
    def _():
        pass_chem.wait_send()
        for copy in pass_phi:
            copy.wait_send()


def flush(n, staged, half, phase_out, chem_out, final, sem):
    cz, nx = staged.shape[1:3]
    early, tiles = cz - LATE, nx // ROWS
    me = lax.axis_index("grow")

    def out(src, low, count, k):
        return (
            pltpu.make_async_copy(src.at[0:4], phase_out.at[:, pl.ds(low, count)], sem.at[0, k]),
            pltpu.make_async_copy(src.at[4:6], chem_out.at[:, pl.ds(low, count)], sem.at[1, k]),
        )

    first_part = out(staged.at[:, 0:early], 0, early, LATE)
    for copy in first_part:
        copy.start()

    def late(q):
        return out(final.at[:, pl.ds(q, 1)], early + q, 1, q)

    def plane(q, _):
        z = q + early + 2

        @pl.when(me < n - 1)
        def _():
            for t in range(tiles):
                new, chem = tile_step(half, z, t, tiles, (me + 1) * cz - 2 + z, n * cz)
                for f, value in enumerate(new + chem):
                    final[f, q, t * ROWS : (t + 1) * ROWS] = value

        @pl.when(me == n - 1)
        def _():
            for f in range(6):
                final[f, q] = staged[f, early + q]

        for copy in late(q):
            copy.start()
        return _

    lax.fori_loop(0, LATE, plane, None)
    for copy in first_part:
        copy.wait()

    def written(q, _):
        for copy in late(q):
            copy.wait()
        return _

    lax.fori_loop(0, LATE, written, None)


def body(labels, seed_blend, potential, inflow_index, liquid_table):
    n, m = lax.axis_size("grow"), lax.axis_size("lat")
    cz, nx, ny = labels.shape
    dma = pltpu.SemaphoreType.DMA
    f32 = jnp.float32
    vmem, hbm = pl.BlockSpec(memory_space=pltpu.VMEM), pl.BlockSpec(memory_space=pltpu.HBM)
    state = pl.pallas_call(
        functools.partial(kernel, n, m),
        out_shape=(pltpu.VMEM((6, cz, nx, ny), f32), pltpu.VMEM((5, cz + 4, nx + ROWS, ny), f32)),
        in_specs=[hbm] * 5,
        out_specs=(vmem, vmem),
        scratch_shapes=[
            pltpu.SMEM(liquid_table.shape[::-1], f32),
            pltpu.VMEM((cz, nx, ny), jnp.int32),
            pltpu.VMEM((4, cz, nx, ny), f32),
            pltpu.VMEM((cz, nx, ny), jnp.int32),
            pltpu.VMEM((3, cz, nx, ny), f32),
            pltpu.VMEM((5, cz + 4, nx + ROWS, ny), f32),
            pltpu.VMEM((5, cz + 4, ROWS, ny), f32),
            pltpu.VMEM((5, cz + 4, ROWS, ny), f32),
            pltpu.VMEM((5, 2, nx, ny), f32),
            dma((5,)),
            dma((18,)),
            dma((17,)),
            dma((cz,)),
            dma((cz,)),
            dma((2, 5 + cz)),
            dma((2, 5 + cz)),
            pltpu.SemaphoreType.REGULAR,
        ],
        compiler_params=pltpu.CompilerParams(collective_id=0, has_side_effects=True, vmem_limit_bytes=12 << 20),
    )(*(pltpu.with_memory_space_constraint(a, pltpu.HBM) for a in (labels, seed_blend, potential, inflow_index, liquid_table.T)))
    return pl.pallas_call(
        functools.partial(flush, n),
        out_shape=(jax.ShapeDtypeStruct((4, cz, nx, ny), f32), jax.ShapeDtypeStruct((2, cz, nx, ny), f32)),
        in_specs=[vmem, vmem],
        out_specs=(hbm, hbm),
        scratch_shapes=[pltpu.VMEM((6, LATE, nx, ny), f32), dma((2, LATE + 1))],
        compiler_params=pltpu.CompilerParams(vmem_limit_bytes=4 << 20),
    )(*(pltpu.with_memory_space_constraint(a, pltpu.VMEM) for a in state))


def solution(mesh):
    in_specs = (
        P("grow", "lat", None),
        P(None, "grow", "lat", None),
        P(None, "grow", "lat", None),
        P(None, "lat", None),
        P(),
    )
    out_specs = (P(None, "grow", "lat", None), P(None, "grow", "lat", None))
    return jax.shard_map(body, mesh=mesh, in_specs=in_specs, out_specs=out_specs, check_vma=False)
```

```python
import functools

import jax
import jax.numpy as jnp
from jax import lax
from jax.experimental import pallas as pl
from jax.experimental.pallas import tpu as pltpu
from jax.sharding import PartitionSpec as P

offset_table = ((0.0, 0.0), (0.6, -0.3), (-0.4, 0.5), (-0.2, -0.6))
latent_heat = (0.0, 0.8, 0.8, 0.8)
relax_rate = 0.1
diffusion = 0.05
MESH = pl.DeviceIdType.MESH
ROWS = 8
LATE = 3


def advance(phi, chem, lap, temp):
    phi = list(phi) + [1.0 - (phi[0] + phi[1] + phi[2])]
    square = chem[0] * chem[0] + chem[1] * chem[1]
    pull = []
    for a in range(4):
        e0, e1 = offset_table[a]
        p = phi[a]
        w = square - (1.0 - p) * (1.0 - 2.0 * p)
        if a:
            w = w + ((2.0 * e0) * chem[0] + (2.0 * e1) * chem[1] + ((e0 * e0 + e1 * e1) - 2.0 * latent_heat[a] * temp))
        pull.append(p * w)
    mean = 0.25 * ((pull[0] + pull[1]) + (pull[2] + pull[3]))
    new = [phi[a] + relax_rate * ((lap[a] + pull[a]) - mean) for a in range(3)]
    new.append(1.0 - (new[0] + new[1] + new[2]))
    squares = [v * v for v in new]
    growth = [squares[a] - phi[a] * phi[a] for a in range(4)]
    total = (growth[0] + growth[1]) + (growth[2] + growth[3])
    inverse = 1.0 / ((squares[0] + squares[1]) + (squares[2] + squares[3]))
    mobile = diffusion * (0.1 + squares[0])
    out = []
    for k in range(2):
        source = chem[k] * total
        for a in range(1, 4):
            source = source + offset_table[a][k] * growth[a]
        out.append(chem[k] + (mobile * lap[3 + k] - source) * inverse)
    return new, out


def tile_step(src, z, t, tiles, plane, planes):
    ny = src.shape[-1]
    row = lax.broadcasted_iota(jnp.int32, (ROWS, ny), 0)

    def part(f, z, t):
        return src[f, z, t * ROWS : (t + 1) * ROWS]

    after, before = (t + 1) % (tiles + 1), (t + tiles) % (tiles + 1)
    centre, lap = [], []
    for f in range(5):
        c = part(f, z, t)
        up = pltpu.roll(jnp.where(row == 0, part(f, z, after), c), ROWS - 1, 0)
        down = pltpu.roll(jnp.where(row == ROWS - 1, part(f, z, before), c), 1, 0)
        lap.append(
            ((part(f, z + 1, t) + part(f, z - 1, t)) + (up + down))
            + (pltpu.roll(c, ny - 1, 1) + pltpu.roll(c, 1, 1)) - 6.0 * c)
        centre.append(c)
    temp = 2.0 * (plane.astype(jnp.float32) + 0.5) / float(planes) - 1.0
    return advance(centre[:3], centre[3:], lap, temp)


PLANE, EDGES, MID, LAST, HEAD, PASS_MID, PASS_LAST, END, END_NEXT, BOTH, CROSS = range(1, 12)


def schedule(kind, cz):
    pair, head, top = cz - 2, cz - 1, cz + 2
    none = (0, 0)

    def step(event, sent=None, landed=None, halo=none, own=none, two=none):
        return (event, 0 if sent is None else sent + 1, 0 if landed is None else landed + 1, halo, own, two)

    if kind == 0:
        return [
            step(PLANE, 0, cz),
            step(PLANE, 1, 0, none, (1, 1)),
            step(PLANE, 2, 1, (2, 1), (2, 1)),
            *(step(PLANE, p, p - 1, (p, 1), (p, 1), (p - 1, 1)) for p in range(3, pair)),
            step(EDGES, pair, pair - 1, (pair, 1), (pair, 1), (pair - 1, 1)),
            step(0, None, pair, (pair + 1, 3)),
            step(MID, None, None, none, (pair + 1, 1), (pair, 1)),
            step(LAST, None, None, none, (cz, 3), (cz - 1, 3)),
        ]
    body = [step(PLANE, 2), step(PLANE, 3, 2)]
    if kind == 1:
        return [
            *body,
            step(PLANE, 4, 3),
            step(PLANE, 5, 4, (5, 1), (5, 1)),
            *(step(PLANE, p, p - 1, (p, 1), (p, 1), (p - 1, 1) if p > 6 else none) for p in range(6, pair)),
            step(EDGES, pair, pair - 1, (pair, 1), (pair, 1), (pair - 1, 1) if pair > 6 else none),
            step(0, None, pair, (pair + 1, 2)),
            step(MID, None, None, none, (pair + 1, 1), (pair, 1)),
            step(LAST, None, None, none, (cz, 1), (cz - 1, 1)),
            step(HEAD, head),
            step(0, None, head, (2, 3)),
            step(PASS_MID, None, None, none, (4, 1), (5, 1)),
            step(PASS_LAST, None, None, none, (1, 3), (2, 3)),
            step(END, cz),
            step(0, None, cz, (cz + 1, 1), (cz + 1, 1), (cz, 1)),
            step(END_NEXT, None, None, none, (top, 1), (cz + 1, 1)),
        ]
    return [
        *body,
        step(END, cz, 3),
        step(PLANE, 4, cz),
        step(END_NEXT, None, 4, (5, 1), (5, 1)),
        step(PLANE, 5),
        *(step(PLANE, p, p - 1, (p, 1), (p, 1), (p - 1, 1) if p > 6 else none) for p in range(6, pair)),
        step(HEAD, head, pair - 1, (pair, 1), (pair, 1), (pair - 1, 1) if pair > 6 else none),
        step(PASS_MID, None, head, (2, 3), (4, 1), (5, 1)),
        step(CROSS, pair, None, none, (1, 3), (2, 3)),
        step(BOTH, None, pair, (pair + 1, 3), (pair + 1, 4), (pair, 4)),
    ]


BASE = 32


def pack(step):
    event, sent, landed, halo, own, two = step
    work = 0
    for low, number in (two, own, halo):
        work = work * (8 * BASE) + low + BASE * number
    return event + BASE * (sent + BASE * landed), work


def pick(k, values):
    bit = 1
    while len(values) > 1:
        odd = k // bit % 2 == 1
        paired = [jnp.where(odd, b, a) for a, b in zip(values[0::2], values[1::2])]
        values = paired + values[len(values) - len(values) % 2 :]
        bit *= 2
    return values[0]


def kernel(n, m, labels_h, blend_h, chem_h, index_h, table_h, staged, half,
           table, labels, blend, index, own, g, from_right, from_left, relay,
           load_sem, send_sem, recv_sem, plane_send, plane_recv, lat_send, lat_recv, go):
    cz, nx, ny = labels.shape
    tiles = nx // ROWS
    inner = tuple(range(tiles))
    top = cz + 2
    me = lax.axis_index("grow")
    lat = lax.axis_index("lat")
    right, left = lax.rem(lat + 1, m), lax.rem(lat + m - 1, m)
    corner = lax.rem(me, 4)
    even = lax.rem(me, 2) == 0
    odd = jnp.logical_not(even)
    gives, gets = me > 0, me < n - 1
    gets_end = me < n - 2
    gives_via = jnp.logical_and(corner == 0, me > 0)
    gets_via = jnp.logical_and(corner == 2, me > 4)
    row = lax.broadcasted_iota(jnp.int32, (ROWS, ny), 0)

    barrier = pltpu.get_barrier_semaphore()

    def greet(there, device):
        @pl.when(there)
        def _():
            pl.semaphore_signal(barrier, inc=1, device_id={"grow": device}, device_id_type=MESH)

    greet(odd, me - 1)
    greet(even, me + 1)
    greet(jnp.logical_and(odd, me + 1 < n), me + 1)
    greet(corner == 0, me + 2)
    greet(gets_via, me - 2)
    greet(jnp.logical_and(corner == 2, me + 4 < n), me + 4)
    for side in (left, right):
        pl.semaphore_signal(barrier, inc=1, device_id={"lat": side}, device_id_type=MESH)

    loads = [
        pltpu.make_async_copy(labels_h, labels, load_sem.at[0]),
        pltpu.make_async_copy(blend_h, blend, load_sem.at[1]),
        pltpu.make_async_copy(index_h, index, load_sem.at[2]),
        pltpu.make_async_copy(chem_h.at[:, cz - 2 : cz], g.at[3:5, 0:2, 0:nx], load_sem.at[3]),
        pltpu.make_async_copy(table_h, table, load_sem.at[4]),
    ]
    for load in loads:
        load.start()

    met = 3 + jnp.where(even, (me > 0).astype(jnp.int32) + (corner == 2).astype(jnp.int32)
                        + gets_via.astype(jnp.int32) + gives_via.astype(jnp.int32), 0)
    pl.semaphore_wait(barrier, met)

    @pl.when(even)
    def _():
        pl.semaphore_signal(go, inc=1, device_id={"grow": me + 1}, device_id_type=MESH)

    def to(step):
        return lax.rem(me + n + step, n)

    def along(src, dst, send, recv, device):
        return pltpu.make_async_remote_copy(
            src_ref=src, dst_ref=dst, send_sem=send_sem.at[send], recv_sem=recv_sem.at[recv],
            device_id={"grow": device}, device_id_type=MESH)

    low, middle, high = pl.ds(0, ROWS), pl.ds(ROWS, nx - 2 * ROWS), pl.ds(nx - ROWS, ROWS)
    rows = pl.ds(0, nx)

    end = (
        along(chem_h.at[:, 0:2], g.at[3:5, top : top + 2, rows], 0, 0, to(-2)),
        along(own.at[:, 0:1], g.at[0:3, top : top + 1, rows], 1, 1, to(-2)),
        along(own.at[:, 1:2], g.at[0:3, top + 1 : top + 2, rows], 2, 2, to(-2)),
    )
    via = (
        along(chem_h.at[:, 0:2], relay.at[3:5], 0, 13, to(2)),
        along(own.at[:, 0:1], relay.at[0:3, 0:1], 1, 14, to(2)),
        along(own.at[:, 1:2], relay.at[0:3, 1:2], 2, 15, to(2)),
    )
    far = (
        along(relay.at[3:5], g.at[3:5, top : top + 2, rows], 13, 0, to(-4)),
        along(relay.at[0:3, 0:1], g.at[0:3, top : top + 1, rows], 14, 1, to(-4)),
        along(relay.at[0:3, 1:2], g.at[0:3, top + 1 : top + 2, rows], 15, 2, to(-4)),
    )
    head_chem = along(chem_h.at[:, 0:2], g.at[3:5, 2:4, rows], 3, 3, to(-1))
    lead_chem = along(chem_h.at[:, 2:4], g.at[3:5, 4:6, rows], 16, 16, to(-1))
    body_chem = along(chem_h.at[:, 4:cz], g.at[3:5, 6:top, rows], 4, 4, to(-1))
    def banded(src, dst, send, recv, device):
        return [
            along(src(planes, band), dst(planes, band), send + k, recv + k, device)
            for k, (planes, band) in enumerate(
                ((pl.ds(0, 2), low), (pl.ds(0, 2), high), (pl.ds(0, 1), middle), (pl.ds(1, 1), middle)))
        ]

    final_own, final_g = own.at[:, cz - 2 : cz], g.at[0:3, cz:top]
    last_phi = banded(lambda p, r: final_own.at[:, p, r], lambda p, r: final_g.at[:, p, r], 5, 5, to(-1))
    end_g, head_g = g.at[0:3, top : top + 2], g.at[0:3, 2:4]
    pass_chem = along(g.at[3:5, top : top + 2, rows], g.at[3:5, 2:4, rows], 17, 3, to(1))
    pass_phi = banded(lambda p, r: end_g.at[:, p, r], lambda p, r: head_g.at[:, p, r], 9, 9, to(1))
    pass_phi = [pass_phi[0], pass_phi[1], pass_phi[3], pass_phi[2]]

    def plane_phi(p):
        return pltpu.make_async_remote_copy(
            src_ref=own.at[:, pl.ds(p, 1)], dst_ref=g.at[0:3, pl.ds(p + 2, 1), rows],
            send_sem=plane_send.at[p], recv_sem=plane_recv.at[p],
            device_id={"grow": to(-1)}, device_id_type=MESH)

    gives_end = jnp.logical_and(me > 1, corner != 0)
    even_end = jnp.logical_and(corner == 2, me > 1)
    odd_end = jnp.logical_and(odd, me > 1)

    @pl.when(odd)
    def _():
        head_chem.start()

    @pl.when(gives)
    def _():
        lead_chem.start()
        body_chem.start()

    @pl.when(even_end)
    def _():
        end[0].start()

    @pl.when(gives_via)
    def _():
        via[0].start()

    loads[0].wait()
    loads[1].wait()

    def initial(p, _):
        kind = labels[p]
        weights = [blend[a, p] for a in range(4)]
        inverse = 1.0 / (1.0 + ((weights[0] + weights[1]) + (weights[2] + weights[3])))
        for a in range(3):
            own[a, p] = (jnp.where(kind == a, 1.0, 0.0) + weights[a]) * inverse
        return _

    lax.fori_loop(0, cz, initial, None)

    @pl.when(odd)
    def _():
        plane_phi(0).start()
        plane_phi(1).start()

    @pl.when(even_end)
    def _():
        end[1].start()
        end[2].start()

    @pl.when(gives_via)
    def _():
        via[1].start()
        via[2].start()

    def planes(low_p, high_p, act):
        def step(p, _):
            act(plane_phi(p))
            return _

        lax.fori_loop(low_p, high_p, step, None)

    @pl.when(gives)
    def _():
        planes(2, cz - 2, lambda copy: copy.start())
        for copy in last_phi:
            copy.start()

    for k in range(2):
        for a in range(3):
            g[a, k, 0:nx] = own[a, cz - 2 + k]

    @pl.when(odd)
    def _():
        pl.semaphore_wait(go, 1)

    loads[2].wait()
    loads[3].wait()
    loads[4].wait()

    @pl.when(gets_via)
    def _():
        for landed, onward in zip(via, far):
            landed.wait_recv()
            onward.start()

    def sideways(fields, planes, group):
        return (
            pltpu.make_async_remote_copy(
                src_ref=g.at[fields, planes, nx - ROWS : nx], dst_ref=from_left.at[fields, planes],
                send_sem=lat_send.at[0, group], recv_sem=lat_recv.at[0, group],
                device_id={"lat": right}, device_id_type=MESH),
            pltpu.make_async_remote_copy(
                src_ref=g.at[fields, planes, 0:ROWS], dst_ref=from_right.at[fields, planes],
                send_sem=lat_send.at[1, group], recv_sem=lat_recv.at[1, group],
                device_id={"lat": left}, device_id_type=MESH),
        )

    everything, phases, chemical = slice(0, 5), slice(0, 3), slice(3, 5)
    lat_own = sideways(everything, slice(1, 2), 0)
    lat_head_chem = sideways(chemical, slice(2, 4), 1)
    lat_end_chem = sideways(chemical, slice(top, top + 1), 2)
    lat_chem = sideways(chemical, slice(4, top), 3)

    lat_pair = sideways(phases, slice(cz, top), 4 + cz - 2)
    lat_head = sideways(phases, slice(2, 4), 4 + cz - 1)

    def lat_plane(p):
        return sideways(phases, pl.ds(p + 2, 1), 4 + p)

    def start(pair):
        for copy in pair:
            copy.start()

    def wait(pair):
        for copy in pair:
            copy.wait()

    def merge(fields, z):
        for f in fields:
            g[f, z, nx : nx + ROWS] = jnp.where(row < 4, from_right[f, z], from_left[f, z])

    def first(z, parts):
        for t in parts:
            new, chem = tile_step(g, z, t, tiles, (me + 1) * cz - 2 + z, n * cz)
            for f, value in enumerate(new[:3] + chem):
                half[f, z, t * ROWS : (t + 1) * ROWS] = value

    def second(z):
        for t in inner:
            new, chem = tile_step(half, z, t, tiles, (me + 1) * cz - 2 + z, n * cz)
            for f, value in enumerate(new + chem):
                staged[f, z - 2, t * ROWS : (t + 1) * ROWS] = value

    def chem_in():
        start(lat_own)
        body_chem.wait_recv()
        start(lat_chem)
        wait(lat_own)
        merge(range(5), 1)
        wait(lat_chem)
        lax.fori_loop(4, top, lambda z, _: merge((3, 4), z), None)

    def head_chem_lands():
        wait(lat_head_chem)
        lax.fori_loop(2, 4, lambda z, _: merge((3, 4), z), None)

    @pl.when(jnp.logical_and(even, gets_end))
    def _():
        end[0].wait_recv()
        pass_chem.start()
        start(lat_end_chem)
        end[1].wait_recv()
        start(lat_plane(cz))
        end[2].wait_recv()
        for copy in pass_phi:
            copy.start()

    @pl.when(gets)
    def _():
        lead_chem.wait_recv()

    @pl.when(odd_end)
    def _():
        for copy in end:
            copy.start()

    @pl.when(gets)
    def _():
        chem_in()

    @pl.when(jnp.logical_and(gets, even))
    def _():
        head_chem.wait_recv()
        start(lat_head_chem)
        head_chem_lands()

    code = jnp.where(even, 0, jnp.where(corner == 1, 1, 2))
    plans = [schedule(kind, cz) for kind in range(3)]
    words = []
    for k in range(max(len(plan) for plan in plans)):
        packed = [pack(plan[k]) if k < len(plan) else (0, 0) for plan in plans]
        words.append([jnp.where(code == 0, p0, jnp.where(code == 1, p1, p2)) for p0, p1, p2 in zip(*packed)])
    count = jnp.where(code == 0, len(plans[0]), jnp.where(code == 1, len(plans[1]), len(plans[2])))
    count = jnp.where(gets, count, 0)
    topmost = jnp.logical_not(gets_end)

    def run(k, _):
        comm, work = pick(k, [w[0] for w in words]), pick(k, [w[1] for w in words])
        event, sent, landed = comm % BASE, comm // BASE % BASE, comm // (BASE * BASE)

        def span(value):
            low_z = value % BASE
            return low_z, low_z + value // BASE

        h0, h1 = span(work % (8 * BASE))
        f0, f1 = span(work // (8 * BASE) % (8 * BASE))
        s0, s1 = span(work // (64 * BASE * BASE))

        @pl.when(event == PLANE)
        def _():
            plane_phi(sent - 1).wait_recv()

        @pl.when(jnp.logical_or(event == EDGES, event == CROSS))
        def _():
            last_phi[0].wait_recv()
            last_phi[1].wait_recv()
            start(lat_pair)

        @pl.when(jnp.logical_or(event == MID, event == BOTH))
        def _():
            last_phi[2].wait_recv()

        @pl.when(jnp.logical_or(event == LAST, event == BOTH))
        def _():
            last_phi[3].wait_recv()

        @pl.when(event == HEAD)
        def _():
            head_chem.wait_recv()
            start(lat_head_chem)
            pass_phi[0].wait_recv()
            pass_phi[1].wait_recv()
            start(lat_head)

        @pl.when(event == PASS_MID)
        def _():
            pass_phi[2].wait_recv()

        @pl.when(jnp.logical_or(event == PASS_LAST, event == CROSS))
        def _():
            pass_phi[3].wait_recv()

        @pl.when(event == END)
        def _():
            end[0].wait_recv()
            start(lat_end_chem)
            end[1].wait_recv()

        @pl.when(event == END_NEXT)
        def _():
            end[2].wait_recv()

        @pl.when(jnp.logical_or(event == PLANE, event == END))
        def _():
            start(lat_plane(sent - 1))

        ending = landed == cz + 1

        @pl.when(jnp.logical_and(ending, gets_end))
        def _():
            wait(lat_end_chem)
            merge((3, 4), top)

        @pl.when(jnp.logical_or(jnp.logical_and(landed > 0, landed < cz - 1), jnp.logical_and(ending, gets_end)))
        def _():
            wait(lat_plane(landed - 1))
            merge(range(3), landed + 1)

        @pl.when(landed == cz - 1)
        def _():
            wait(lat_pair)
            lax.fori_loop(cz, top, lambda z, _: merge(range(3), z), None)

        @pl.when(landed == cz)
        def _():
            head_chem_lands()
            wait(lat_head)
            lax.fori_loop(2, 4, lambda z, _: merge(range(3), z), None)

        @pl.when(jnp.logical_and(topmost, landed == cz - 1))
        def _():
            for f in range(5):
                g[f, top, nx:] = g[f, top - 1, nx:]

        @pl.when(jnp.logical_and(topmost, event == LAST))
        def _():
            for f in range(5):
                g[f, top, 0:nx] = g[f, top - 1, 0:nx]

        def halo_pair(q, _):
            for step in range(2):
                first(h0 + 2 * q + step, (tiles,))
            return _

        lax.fori_loop(0, (h1 - h0) // 2, halo_pair, None)
        lax.fori_loop(h1 - (h1 - h0) % 2, h1, lambda z, _: first(z, (tiles,)), None)
        lax.fori_loop(f0, jnp.minimum(f1, jnp.where(topmost, top, top + 1)), lambda z, _: first(z, inner), None)

        @pl.when(jnp.logical_and(topmost, event == LAST))
        def _():
            for f in range(5):
                half[f, top, 0:nx] = half[f, top - 1, 0:nx]

        lax.fori_loop(s0, jnp.minimum(s1, cz + 2 - LATE), lambda z, _: second(z), None)
        return _

    lax.fori_loop(0, count, run, None)

    @pl.when(jnp.logical_not(gets))
    def _():
        def entering(o, _):
            kind = index[o]
            for a in range(4):
                staged[a, o] = jnp.full((nx, ny), 1.0 if a == 0 else 0.0, jnp.float32)
            for k in range(2):
                value = jnp.zeros((nx, ny), jnp.float32)
                for liquid in range(table.shape[1]):
                    value = jnp.where(kind == liquid, table[k, liquid], value)
                staged[4 + k, o] = value
            return _

        lax.fori_loop(0, cz, entering, None)

    @pl.when(gives_end)
    def _():
        for copy in end:
            copy.wait_send()

    @pl.when(gives_via)
    def _():
        for copy in via:
            copy.wait_send()

    @pl.when(gets_via)
    def _():
        for copy in far:
            copy.wait_send()

    @pl.when(odd)
    def _():
        head_chem.wait_send()
        plane_phi(0).wait_send()
        plane_phi(1).wait_send()

    @pl.when(gives)
    def _():
        lead_chem.wait_send()
        body_chem.wait_send()
        planes(2, cz - 2, lambda copy: copy.wait_send())
        for copy in last_phi:
            copy.wait_send()

    @pl.when(jnp.logical_and(even, gets_end))
    def _():
        pass_chem.wait_send()
        for copy in pass_phi:
            copy.wait_send()


def flush(n, staged, half, phase_out, chem_out, final, sem):
    cz, nx = staged.shape[1:3]
    early, tiles = cz - LATE, nx // ROWS
    me = lax.axis_index("grow")

    def out(src, low, count, k):
        return (
            pltpu.make_async_copy(src.at[0:4], phase_out.at[:, pl.ds(low, count)], sem.at[0, k]),
            pltpu.make_async_copy(src.at[4:6], chem_out.at[:, pl.ds(low, count)], sem.at[1, k]),
        )

    first_part = out(staged.at[:, 0:early], 0, early, LATE)
    for copy in first_part:
        copy.start()

    def late(q):
        return out(final.at[:, pl.ds(q, 1)], early + q, 1, q)

    def plane(q, _):
        z = q + early + 2

        @pl.when(me < n - 1)
        def _():
            for t in range(tiles):
                new, chem = tile_step(half, z, t, tiles, (me + 1) * cz - 2 + z, n * cz)
                for f, value in enumerate(new + chem):
                    final[f, q, t * ROWS : (t + 1) * ROWS] = value

        @pl.when(me == n - 1)
        def _():
            for f in range(6):
                final[f, q] = staged[f, early + q]

        for copy in late(q):
            copy.start()
        return _

    lax.fori_loop(0, LATE, plane, None)
    for copy in first_part:
        copy.wait()

    def written(q, _):
        for copy in late(q):
            copy.wait()
        return _

    lax.fori_loop(0, LATE, written, None)


def body(labels, seed_blend, potential, inflow_index, liquid_table):
    n, m = lax.axis_size("grow"), lax.axis_size("lat")
    cz, nx, ny = labels.shape
    dma = pltpu.SemaphoreType.DMA
    f32 = jnp.float32
    vmem, hbm = pl.BlockSpec(memory_space=pltpu.VMEM), pl.BlockSpec(memory_space=pltpu.HBM)
    state = pl.pallas_call(
        functools.partial(kernel, n, m),
        out_shape=(pltpu.VMEM((6, cz, nx, ny), f32), pltpu.VMEM((5, cz + 4, nx + ROWS, ny), f32)),
        in_specs=[hbm] * 5,
        out_specs=(vmem, vmem),
        scratch_shapes=[
            pltpu.SMEM(liquid_table.shape[::-1], f32),
            pltpu.VMEM((cz, nx, ny), jnp.int32),
            pltpu.VMEM((4, cz, nx, ny), f32),
            pltpu.VMEM((cz, nx, ny), jnp.int32),
            pltpu.VMEM((3, cz, nx, ny), f32),
            pltpu.VMEM((5, cz + 4, nx + ROWS, ny), f32),
            pltpu.VMEM((5, cz + 4, ROWS, ny), f32),
            pltpu.VMEM((5, cz + 4, ROWS, ny), f32),
            pltpu.VMEM((5, 2, nx, ny), f32),
            dma((5,)),
            dma((18,)),
            dma((17,)),
            dma((cz,)),
            dma((cz,)),
            dma((2, 5 + cz)),
            dma((2, 5 + cz)),
            pltpu.SemaphoreType.REGULAR,
        ],
        compiler_params=pltpu.CompilerParams(collective_id=0, has_side_effects=True, vmem_limit_bytes=12 << 20),
    )(*(pltpu.with_memory_space_constraint(a, pltpu.HBM) for a in (labels, seed_blend, potential, inflow_index, liquid_table.T)))
    return pl.pallas_call(
        functools.partial(flush, n),
        out_shape=(jax.ShapeDtypeStruct((4, cz, nx, ny), f32), jax.ShapeDtypeStruct((2, cz, nx, ny), f32)),
        in_specs=[vmem, vmem],
        out_specs=(hbm, hbm),
        scratch_shapes=[pltpu.VMEM((6, LATE, nx, ny), f32), dma((2, LATE + 1))],
        compiler_params=pltpu.CompilerParams(vmem_limit_bytes=4 << 20),
    )(*(pltpu.with_memory_space_constraint(a, pltpu.VMEM) for a in state))


def solution(mesh):
    in_specs = (
        P("grow", "lat", None),
        P(None, "grow", "lat", None),
        P(None, "grow", "lat", None),
        P(None, "lat", None),
        P(),
    )
    out_specs = (P(None, "grow", "lat", None), P(None, "grow", "lat", None))
    return jax.shard_map(body, mesh=mesh, in_specs=in_specs, out_specs=out_specs, check_vma=False)
```
